128 devices in a mesh: gx: 32 (over y, z, core), gy: 4 (over x).
Axes of the slice: x: 4, y: 4, z: 4, core: 2. Of those that a mesh axis runs over, the one named last changes fastest.
Arguments:
- vorticity_grid: float32 [4096, 4096], P(('gx', 'gy')), may hold values from -6 to 6
- forcing_grid: float32 [4096, 4096], P(('gx', 'gy')), may hold values from -12 to 12
- cutoff: int32 [1], replicated, may hold values from 853 to 1365
- forcing_shells: int32 [4], replicated, may hold values from 2 to 127
Outputs:
- lifted_spectrum: float32 [2, 4096, 4096], P(None, ('gx', 'gy'))
- coarse_field: float32 [256, 256], P(('gx', 'gy'))
The draws below stay inside these ranges and needn't reach their ends.
Inputs may be any that keep to these rules, and one draw needn't show every extreme that they name: Nonlinear modes with an absolute wavenumber index above cutoff are removed.
All inputs are finite; a program needn't handle non-finite values.
Results may differ from the reference program's by a relative error of at most 0.0001.
Values sent between devices are 32-bit elements; how exact they have to be, the bound alone decides.
No kernel may reach another device: no remote copies, remote signals or barrier semaphores. Data moves between devices by JAX's collectives and lax.ppermute only.
A program may use at most 128 MiB of HBM per device.

```python
import math
import jax
import jax.numpy as jnp

GRID = 4096
STEPS = 1
LOW = 256
SHELLS = 4


def with_ends(array, rng, least, high):
    longest = array.shape.index(max(array.shape))
    spots = []
    for shift in (0, 1):
        where = [jax.random.randint(jax.random.fold_in(rng, axis), (), 0, length) for axis, length in enumerate(array.shape)]
        where[longest] = (where[longest] + shift) % array.shape[longest]
        spots.append(tuple(where))
    return array.at[spots[0]].set(least).at[spots[1]].set(high)


def levels(rng, shape, shards, least, high):
    loudness, own = 1.0, jax.random.fold_in(rng, 6)
    for position, shards_of in shards:
        steps = jnp.exp(jax.random.uniform(jax.random.fold_in(own, position), (shards_of,), jnp.float32, least / len(shards), high / len(shards)))
        loudness = loudness * jnp.repeat(steps, shape[position] // shards_of).reshape([-1 if axis == position else 1 for axis in range(len(shape))])
    return loudness


def centred(rng, shape, deviation, reach, cuts=(), kind=jnp.bfloat16):
    factor_of = levels(rng, shape, cuts, -0.22, 0.18) if cuts else 1.0
    values = jax.random.normal(rng, shape, jnp.float32) * deviation * factor_of
    return jnp.minimum(jnp.maximum(values, -reach), reach).astype(kind)


def setup_inputs(seed: int = 0) -> dict:
    keys = jax.random.split(jax.random.key(seed), 5)
    vorticity_grid = centred(keys[0], (GRID, GRID), 1.0, 6.0, ((0, 128),), jnp.float32)
    forcing_grid = centred(keys[1], (GRID, GRID), 2.0, 12.0, ((0, 128),), jnp.float32)
    cutoff = jax.random.randint(keys[2], (1,), GRID // 3 - GRID // 8, GRID // 3 + 1).astype(jnp.int32)
    forcing_shells = with_ends(jax.random.randint(keys[3], (SHELLS,), 2, LOW // 2), jax.random.fold_in(keys[3], 1), 2, (LOW // 2) - 1).astype(jnp.int32)
    return dict(vorticity_grid=vorticity_grid, forcing_grid=forcing_grid, cutoff=cutoff, forcing_shells=forcing_shells)


time_step = 0.05
viscosity = 0.05
coarse_ratio = 4.0


def signed_index(index_array, length_of):
    return jnp.where(index_array < length_of // 2, index_array, index_array - length_of)


def to_spectrum(physical):
    return jnp.fft.fft2(physical, norm="ortho").T


def to_grid(spectrum):
    return jnp.fft.ifft2(spectrum.T, norm="ortho")


def reference(vorticity_grid, forcing_grid, cutoff, forcing_shells):
    indices = jnp.arange(GRID, dtype=jnp.int32)
    wave_y = signed_index(indices, GRID)[:, None]
    wave_x = signed_index(indices, GRID)[None, :]
    wave_unit = 2.0 * math.pi / GRID
    deriv_y = jnp.where(indices[:, None] == GRID // 2, 0, wave_y).astype(jnp.float32) * wave_unit
    deriv_x = jnp.where(indices[None, :] == GRID // 2, 0, wave_x).astype(jnp.float32) * wave_unit
    squares = wave_x * wave_x + wave_y * wave_y
    laplace = squares.astype(jnp.float32) * (wave_unit * wave_unit)
    inverse_lap = jnp.where(squares == 0, 0.0, 1.0 / jnp.maximum(laplace, wave_unit * wave_unit))
    dealias = (jnp.abs(wave_x) <= cutoff[0]) & (jnp.abs(wave_y) <= cutoff[0])
    shell_mask = jnp.zeros((GRID, GRID), dtype=bool)
    for shell_index in range(SHELLS):
        radius = forcing_shells[shell_index]
        shell_mask = shell_mask | ((radius * radius <= squares) & (squares < (radius + 1) * (radius + 1)))
    drive = jnp.where(shell_mask, to_spectrum(forcing_grid), 0.0)
    vorticity = to_spectrum(vorticity_grid)

    def tendency(state):
        stream = state * inverse_lap
        velocity_u = to_grid(1j * deriv_y * stream).real
        velocity_v = to_grid(-1j * deriv_x * stream).real
        grad_x = to_grid(1j * deriv_x * state).real
        grad_y = to_grid(1j * deriv_y * state).real
        advect = velocity_u * grad_x + velocity_v * grad_y
        nonlinear = jnp.where(dealias, to_spectrum(advect), 0.0)
        return -nonlinear - viscosity * laplace * state + drive

    earlier = vorticity
    for step_index in range(STEPS):
        earlier = vorticity
        first_slope = tendency(vorticity)
        second_slope = tendency(vorticity + time_step * first_slope)
        vorticity = vorticity + 0.5 * time_step * (first_slope + second_slope)
    projected = vorticity + coarse_ratio * (vorticity - earlier)
    half_low = LOW // 2
    low_modes = (wave_x >= -half_low) & (wave_x < half_low) & (wave_y >= -half_low) & (wave_y < half_low)
    lifted = jnp.where(low_modes, projected, vorticity)
    block_rows = jnp.concatenate([projected[:half_low], projected[GRID - half_low:]], axis=0)
    block_low = jnp.concatenate([block_rows[:, :half_low], block_rows[:, GRID - half_low:]], axis=1)
    coarse = jnp.fft.ifft2(block_low.T, norm="ortho").real
    return jnp.stack([lifted.real, lifted.imag]), coarse
```

```python
import functools
import math

import jax
import jax.numpy as jnp
import numpy as np
from jax import lax
from jax.experimental import pallas as pl
from jax.experimental.pallas import tpu as pltpu
from jax.sharding import PartitionSpec as P

GRID = 4096
LANES = 128
LOW = 256
SHELLS = 4
VMEM_LIMIT = 24
AXES = ("gx", "gy")

time_step = 0.05
viscosity = 0.05
coarse_ratio = 4.0
unit = 2.0 * math.pi / GRID


def split_np(table, axis):
    high = table.astype(np.float32).astype(jnp.bfloat16)
    low = (table - high.astype(np.float64)).astype(np.float32).astype(jnp.bfloat16)
    return np.concatenate([high, low], axis=axis)


@functools.lru_cache(None)
def tables():
    made = {}
    index = np.arange(128)
    rows = index[:, None]
    angle = 2 * np.pi * np.outer(index, index) / 128
    cos, sin = np.cos(angle) / 8, np.sin(angle) / 8
    made["left"] = split_np(np.block([[cos, sin], [-sin, cos]]), 1)

    lane = np.arange(128)
    inner = 8 * (lane >> 5) + (lane & 7)
    slot = (lane >> 3) & 3
    same = slot[:, None] == slot[None, :]
    angle = 2 * np.pi * np.outer(inner, inner) / 32
    cos, sin = same * np.cos(angle) / 8, same * np.sin(angle) / 8
    made["right_x"] = split_np(np.block([[cos, -sin], [sin, cos]]), 0)

    wide = np.arange(256)
    col_j, col_x = wide >> 3, wide & 7
    out_t, out_x = lane >> 3, lane & 7
    same = col_x[:, None] == out_x[None, :]
    angle = 2 * np.pi * np.outer(col_j, out_t) / 32
    part0 = np.cos(angle)
    part1 = -np.sin(angle)
    part1[:, out_t == 0] = np.where(col_j % 2 == 0, 1.0, -1.0)[:, None]
    right_y = np.concatenate([same * part0, same * part1], axis=1) / 8
    made["forward_y"] = split_np(right_y, 0)
    made["inverse_y"] = split_np(right_y.T, 0)

    turn = 2 * np.pi * rows * inner[None, :] / GRID
    made["turn_x"] = planes([np.cos(turn), np.sin(turn)])
    turn_d = 2 * np.pi * rows * out_t[None, :] / GRID
    back = np.where(out_t == 0, 16, 32 - out_t)
    turn_m = 2 * np.pi * rows * back[None, :] / GRID
    made["turn_y"] = planes([np.cos(turn_d), np.sin(turn_d), np.cos(turn_m), np.sin(turn_m)])
    half = 2 * np.pi * rows / 256 + np.zeros((128, 128))
    made["half"] = planes([np.cos(half), np.sin(half)])

    angle = 2 * np.pi * np.outer(index, index) / GRID
    low = np.concatenate([np.cos(angle), -np.sin(angle)], axis=0) / 64
    made["low_rows"] = split_np(low, 1)
    turn = 2 * np.pi * rows * out_t[None, :] / 32
    made["turn_low"] = planes([np.cos(turn), np.sin(turn)])

    grid = np.arange(512)
    t, group, part, source = grid >> 5, (grid >> 4) & 1, (grid >> 3) & 1, grid & 7
    number = np.where(group == 0, t, np.where(t == 0, 16, 32 - t))
    wave = 32 * source + number
    point = np.arange(LOW)[None, :]
    angle = 2 * np.pi * (wave[:, None] * point % LOW) / LOW
    weight = np.where(wave == 0, 1.0, np.where(wave < 128, 2.0, 0.0))
    weight = np.where((wave == 128) & (part == 0), 1.0, weight)
    value = np.where(part[:, None] == 0, np.cos(angle), -np.sin(angle))
    made["coarse_y"] = split_np(weight[:, None] * value, 0)
    away = np.arange(128)[:, None]
    own = np.arange(32)[None, :]
    parts = []
    for odd in range(2):
        place = 32 * away + 16 * odd - own
        kernel = 1.0 + 2.0 * sum(
            np.cos(2 * np.pi * (p * place % GRID) / GRID) for p in range(1, 128)
        )
        sign = 1.0 - 2.0 * odd
        edge = 2 * np.pi * own / 32 + 0 * away
        parts.append(
            np.concatenate([kernel + sign * np.cos(edge), sign * np.sin(edge)], axis=1)
        )
    scale = -(1 + coarse_ratio) * 0.5 * time_step / (64 * LOW)
    both = np.concatenate(parts, axis=0) * scale
    both = split_np(both, 1)
    high, low = both[:, :64], both[:, 64:]
    made["coarse_x"] = np.concatenate([high, high, low, 0 * low], axis=1)
    return made


def planes(parts):
    return np.concatenate(parts, axis=0).astype(np.float32)


def halves(values):
    high = values.astype(jnp.bfloat16)
    low = (values - high.astype(jnp.float32)).astype(jnp.bfloat16)
    return high, low


def dot(left_side, right_side):
    return jnp.dot(left_side, right_side, preferred_element_type=jnp.float32)


def thrice(table, axis):
    size = table.shape[axis] // 2
    high = lax.slice_in_dim(table, 0, size, axis=axis)
    low = lax.slice_in_dim(table, size, 2 * size, axis=axis)
    return jnp.concatenate([high, high, low], axis=axis)


def left_many(left_table, real, imag):
    count = len(real)
    stacked = jnp.concatenate(
        [jnp.concatenate(real, axis=1), jnp.concatenate(imag, axis=1)], axis=0
    )
    high, low = halves(stacked)
    out = dot(thrice(left_table, 1), jnp.concatenate([high, low, high], axis=0))
    cut = lambda row, place: out[row : row + 128, 128 * place : 128 * place + 128]
    return [cut(0, k) for k in range(count)], [cut(128, k) for k in range(count)]


def right_many(right_table, first, second):
    count = len(first)
    stacked = jnp.concatenate(
        [jnp.concatenate([a, b], axis=1) for a, b in zip(first, second)], axis=0
    )
    high, low = halves(stacked)
    out = dot(jnp.concatenate([high, low, high], axis=1), thrice(right_table, 0))
    cut = lambda row, col: out[128 * row : 128 * row + 128, col : col + 128]
    return [cut(k, 0) for k in range(count)], [cut(k, 128) for k in range(count)]


def lane_ids():
    return lax.broadcasted_iota(jnp.int32, (128, 128), 1)


def row_ids():
    return lax.broadcasted_iota(jnp.int32, (128, 128), 0)


def roll(block, shift):
    shift = shift % 128
    return block if shift == 0 else pltpu.roll(block, shift, 1)


def swap4(blocks):
    lane = lax.broadcasted_iota(jnp.int32, blocks[0].shape, 1)
    out = list(blocks)
    for bit, shift in ((0, 32), (1, 64)):
        low = ((lane >> (5 + bit)) & 1) == 0
        made = list(out)
        for index in range(4):
            if (index >> bit) & 1 == 0:
                a, b = out[index], out[index | (1 << bit)]
                made[index] = jnp.where(low, a, roll(b, shift))
                made[index | (1 << bit)] = jnp.where(low, roll(a, -shift), b)
        out = made
    return out


def turned(real, imag, cos, sin):
    return real * cos + imag * sin, imag * cos - real * sin


class Tables:
    def __init__(self, names, refs):
        self.refs = dict(zip(names, refs))

    def __getitem__(self, name):
        return self.refs[name][...]

    def turn(self, name, index):
        return self.refs[name][128 * index : 128 * index + 128, :]


def x_turned(tab, first, second):
    cos, sin = tab.turn("turn_x", 0), tab.turn("turn_x", 1)
    pairs = [turned(a, b, cos, sin) for a, b in zip(first, second)]
    return [p[0] for p in pairs], [p[1] for p in pairs]


def x_plain(tab, real, imag):
    real, imag = left_many(tab["left"], real, imag)
    return right_many(tab["right_x"], *x_turned(tab, real, imag))


def x_forward(tab, real, imag):
    return x_plain(tab, swap4(real), swap4(imag))


def x_inverse(tab, real, imag):
    first, second = right_many(tab["right_x"], imag, real)
    first, second = left_many(tab["left"], *x_turned(tab, first, second))
    return second, first


def y_forward(tab, groups):
    part0, part1 = right_many(
        tab["forward_y"], [g[0] for g in groups], [g[1] for g in groups]
    )
    start = lane_ids() < 8
    cos, sin = tab.turn("turn_y", 0), tab.turn("turn_y", 1)
    rest = jnp.where(start, 0.0, cos)
    real = [p * cos + q * sin for p, q in zip(part0, part1)]
    imag = [q * rest - p * sin for p, q in zip(part0, part1)]
    direct = left_many(tab["left"], real, imag)
    cos, sin = tab.turn("turn_y", 2), tab.turn("turn_y", 3)
    a, b = jnp.where(start, 0.0, cos), jnp.where(start, cos, -sin)
    d, e = jnp.where(start, 0.0, -sin), jnp.where(start, -sin, -cos)
    real = [p * a + q * b for p, q in zip(part0, part1)]
    imag = [p * d + q * e for p, q in zip(part0, part1)]
    mirror = left_many(tab["left"], real, imag)
    return direct, mirror


def y_inverse(tab, real, imag, last, place):
    imag, real = left_many(tab["left"], imag, real)
    start = lane_ids() < 8
    cos, sin = tab.turn("turn_y", 0), tab.turn("turn_y", 1)
    cos = jnp.where(start, cos, 2.0 * cos)
    sin = 2.0 * sin
    part0 = [p * cos - q * sin for p, q in zip(real, imag)]
    part1 = [p * sin + q * cos for p, q in zip(real, imag)]
    part1 = [
        jnp.where(start, roll(last, -(32 * xh + 8 * place)), part1[xh]) for xh in range(4)
    ]
    return right_many(tab["inverse_y"], part0, part1)


def last_row(tab, real, imag):
    imag, real = left_many(tab["left"], [imag], [real])
    return real[0] * tab.turn("half", 0) - imag[0] * tab.turn("half", 1)


def load(ref, index, count):
    return ref[pl.ds(index, 128, stride=count), :]


def store(ref, index, count, block):
    ref[pl.ds(index, 128, stride=count), :] = block


def load_set(ref, base, count):
    real = [load(ref, base + k, count) for k in range(4)]
    imag = [load(ref, base + 4 + k, count) for k in range(4)]
    return real, imag


def store_set(ref, base, count, real, imag):
    for k in range(4):
        store(ref, base + k, count, real[k])
        store(ref, base + 4 + k, count, imag[k])


def block(ref, index):
    return ref[128 * index : 128 * index + 128, :]


def put(ref, index, value):
    ref[128 * index : 128 * index + 128, :] = value


class Waves:
    def __init__(self, rank, group, quarter):
        lane = lane_ids()
        column = row_ids() + 128 * (8 * (lane >> 5) + (lane & 7))
        slot = 4 * quarter + ((lane >> 3) & 3)
        if group == 1:
            slot = jnp.where(slot == 0, 16, 32 - slot)
        row = 32 * rank + slot
        self.mx = jnp.where(column < GRID // 2, column, column - GRID)
        self.my = jnp.where(row < GRID // 2, row, row - GRID)
        self.squares = self.mx * self.mx + self.my * self.my
        self.lap = self.squares.astype(jnp.float32) * (unit * unit)
        self.dx = jnp.where(column == GRID // 2, 0, self.mx).astype(jnp.float32) * unit
        self.dy = jnp.where(row == GRID // 2, 0, self.my).astype(jnp.float32) * unit

    def inverse_lap(self):
        return jnp.where(
            self.squares == 0, 0.0, 1.0 / jnp.maximum(self.lap, unit * unit)
        )

    def keep(self, cutoff):
        return (jnp.abs(self.mx) <= cutoff) & (jnp.abs(self.my) <= cutoff)

    def shell(self, radii):
        mask = None
        for radius in radii:
            inside = (radius * radius <= self.squares) & (
                self.squares < (radius + 1) * (radius + 1)
            )
            mask = inside if mask is None else mask | inside
        return mask

    def low(self):
        half = LOW // 2
        return (self.mx >= -half) & (self.mx < half) & (self.my >= -half) & (self.my < half)


def send_fields(tab, rank, state, out_ref, count, names, extra=None):
    total = len(names)
    last_real, last_imag = None, None
    lane_slot = (lane_ids() >> 3) & 3
    waves = [Waves(rank, 0, q) for q in range(4)] + [Waves(rank, 1, 0)]
    for place, name in enumerate(names):
        reals, imags = [], []
        for index in range(5):
            wave = waves[index]
            real, imag = state(0, index) if index < 4 else state(1, 0)
            if name in ("u", "v"):
                scale = wave.inverse_lap()
                real, imag = real * scale, imag * scale
            factor = {"u": wave.dy, "v": -wave.dx, "wx": wave.dx, "wy": wave.dy}[name]
            reals.append(-imag * factor)
            imags.append(real * factor)
        mine = lane_slot == place
        moved = roll(reals[4], 8 * place), roll(imags[4], 8 * place)
        last_real = jnp.where(mine, moved[0], 0.0 if last_real is None else last_real)
        last_imag = jnp.where(mine, moved[1], 0.0 if last_imag is None else last_imag)
        real, imag = x_inverse(tab, reals[:4], imags[:4])
        store_set(out_ref, 8 * place, count, swap4(real), swap4(imag))
    real, imag = x_inverse(tab, [last_real], [last_imag])
    real, imag = real[0], imag[0]
    if extra is not None:
        real, imag = extra(real, 0), extra(imag, 1)
    store(out_ref, 8 * total, count, real)
    store(out_ref, 8 * total + 1, count, imag)


FIRST = ("left", "forward_y", "turn_y", "low_rows", "turn_low")
WAVES = ("left", "right_x", "turn_x")
MIDDLE = ("left", "right_x", "turn_x", "half")
ROWS = ("left", "forward_y", "inverse_y", "turn_y", "half")
LAST = ROWS + ("coarse_y", "coarse_x")


def grid_groups(ref):
    groups = []
    for xh in range(4):
        pair = []
        for jh in range(2):
            pieces = [
                ref[8 * xh : 8 * xh + 8, 128 * j : 128 * j + 128]
                for j in range(16 * jh, 16 * jh + 16)
            ]
            pair.append(jnp.concatenate(pieces, axis=0).T)
        groups.append(pair)
    return groups


def first_kernel(vorticity_ref, forcing_ref, *rest):
    tab = Tables(FIRST, rest)
    out_ref = rest[len(FIRST)]
    direct, mirror = y_forward(tab, grid_groups(vorticity_ref))
    store_set(out_ref, 0, 17, *direct)
    store_set(out_ref, 8, 17, *mirror)
    groups = grid_groups(forcing_ref)
    values = jnp.concatenate([g[k] for g in groups for k in range(2)], axis=1)
    high, low = halves(values)
    out = dot(thrice(tab["low_rows"], 1), jnp.concatenate([high, low, high], axis=0))
    lane, row = lane_ids(), row_ids()
    sign = jnp.where((row & 1) == 0, 1.0, -1.0)
    cos, sin = tab.turn("turn_low", 0), tab.turn("turn_low", 1)
    packed = jnp.zeros((128, 128), jnp.float32)
    for xh in range(4):
        at = 256 * xh
        real = out[:128, at : at + 128] + sign * out[:128, at + 128 : at + 256]
        imag = out[128:, at : at + 128] + sign * out[128:, at + 128 : at + 256]
        for part, value in enumerate(turned(real, imag, cos, sin)):
            for shift in (64, 32, 16, 8):
                value = value + roll(value, shift)
            mine = ((lane >> 5) == xh) & (((lane >> 3) & 3) == part)
            packed = jnp.where(mine, value, packed)
    store(out_ref, 16, 17, packed)


def start_kernel(scalars, in_ref, *rest):
    tab = Tables(WAVES, rest)
    state_ref, out_ref = rest[len(WAVES) :]
    rank = scalars[0]
    for group in range(2):
        real, imag = x_forward(tab, *load_set(in_ref, 8 * group, 17))
        for q in range(4):
            put(state_ref, 8 * group + 2 * q, real[q])
            put(state_ref, 8 * group + 2 * q + 1, imag[q])
    row = load(in_ref, 16, 17)
    lane = lane_ids()
    part = (lane >> 3) & 3
    real = jnp.where(part == 0, row, jnp.where(part == 1, roll(row, 8), 0.0))
    imag = jnp.where(part == 0, roll(row, -8), jnp.where(part == 1, -row, 0.0))
    real, imag = x_plain(tab, [real], [imag])

    def extra(values, which):
        source = (real, imag)[which][0]
        for spot, origin in enumerate((0, 103, 8, 111)):
            moved = roll(source, 24 + spot - origin)
            values = jnp.where(lane == 24 + spot, moved, values)
        return values

    state = lambda group, q: (
        block(state_ref, 8 * group + 2 * q),
        block(state_ref, 8 * group + 2 * q + 1),
    )
    send_fields(tab, rank, state, out_ref, 26, ("u", "v", "wx"), extra)


def product_one(tab, in_ref, count, last, place):
    real, imag = load_set(in_ref, 8 * place, count)
    return y_inverse(tab, real, imag, last, place)


def drive_rows(real, imag):
    lane = lane_ids()
    columns = jnp.where(lane < 4, roll(real, -24), roll(imag, -20)).T
    pick = lambda index: jnp.broadcast_to(columns[index : index + 1, :], (8, 128))
    plus = swap4([pick(4 * part + k) for part in range(2) for k in range(2)])
    minus = swap4([pick(4 * part + 2 + k) for part in range(2) for k in range(2)])
    sub = lax.broadcasted_iota(jnp.int32, (8, 128), 0)
    start = (lax.broadcasted_iota(jnp.int32, (8, 128), 1) & 31) == 0
    top = jnp.zeros((8, 128), jnp.float32)
    bottom = jnp.zeros((8, 128), jnp.float32)
    for k in range(4):
        top = jnp.where(sub == k, plus[k], top)
        after = minus[k + 1] if k < 3 else 0.0
        bottom = jnp.where(sub == 7 - k, jnp.where(start, after, minus[k]), bottom)
    return jnp.concatenate([top, jnp.zeros((112, 128), jnp.float32), bottom], axis=0)


def product_first_kernel(in_ref, local_ref, *rest):
    tab = Tables(ROWS, rest)
    out_ref = rest[len(ROWS)]
    last_real, last_imag = load(in_ref, 24, 26), load(in_ref, 25, 26)
    store(out_ref, 16, 17, drive_rows(last_real, last_imag))
    last = last_row(tab, last_real, last_imag)
    u0, u1 = product_one(tab, in_ref, 26, last, 0)
    x0, x1 = product_one(tab, in_ref, 26, last, 2)
    sum0 = [a * b for a, b in zip(u0, x0)]
    sum1 = [a * b for a, b in zip(u1, x1)]
    lane = lane_ids()
    row = 32 * row_ids() + (lane >> 3)
    slope = jnp.where(row < GRID // 2, row, row - GRID)
    slope = jnp.where(row == GRID // 2, 0, slope).astype(jnp.float32) * unit
    real, imag = load_set(local_ref, 0, 17)
    real, imag = [-b * slope for b in imag], [a * slope for a in real]
    row = 32 * row_ids() + 16
    slope = jnp.where(row < GRID // 2, row, row - GRID).astype(jnp.float32) * unit
    last_real, last_imag = 0.0, 0.0
    for xh in range(4):
        mine = (lane >> 3) == 4 * xh
        a, b = load(local_ref, 8 + xh, 17), load(local_ref, 12 + xh, 17)
        last_real = jnp.where(mine, roll(-b * slope, 32 * xh), last_real)
        last_imag = jnp.where(mine, roll(a * slope, 32 * xh), last_imag)
    own = last_row(tab, last_real, last_imag)
    y0, y1 = y_inverse(tab, real, imag, own, 0)
    v0, v1 = product_one(tab, in_ref, 26, last, 1)
    sum0 = [s + a * b for s, a, b in zip(sum0, v0, y0)]
    sum1 = [s + a * b for s, a, b in zip(sum1, v1, y1)]
    direct, mirror = y_forward(tab, list(zip(sum0, sum1)))
    store_set(out_ref, 0, 17, *direct)
    store_set(out_ref, 8, 17, *mirror)


def product_kernel(scalars, in_ref, *rest):
    tab = Tables(LAST, rest)
    out_ref, mixed_ref = rest[len(LAST) :]
    got = load(in_ref, 34, 35)
    mixed_ref[0:4, :] = got[0:4, :]
    mixed_ref[4:8, :] = got[124:128, :]
    last = last_row(tab, load(in_ref, 32, 35), load(in_ref, 33, 35))
    sum0, sum1 = None, None
    for one, two in ((0, 2), (1, 3)):
        a0, a1 = product_one(tab, in_ref, 35, last, one)
        b0, b1 = product_one(tab, in_ref, 35, last, two)
        made0 = [a * b for a, b in zip(a0, b0)]
        made1 = [a * b for a, b in zip(a1, b1)]
        sum0 = made0 if sum0 is None else [s + m for s, m in zip(sum0, made0)]
        sum1 = made1 if sum1 is None else [s + m for s, m in zip(sum1, made1)]
    direct, mirror = y_forward(tab, list(zip(sum0, sum1)))
    store_set(out_ref, 0, 20, *direct)
    store_set(out_ref, 8, 20, *mirror)
    pieces = []
    for xh in range(4):
        for part in (direct[0], direct[1], mirror[0], mirror[1]):
            pieces.append(part[xh][0:8, :])
    across = jnp.concatenate(pieces, axis=0).T
    made = [
        swap4([across[8 * t : 8 * t + 8, :] for t in range(4 * tq, 4 * tq + 4)])
        for tq in range(4)
    ]
    values = jnp.concatenate(
        [jnp.concatenate([made[tq][xh] for tq in range(4)], axis=1) for xh in range(4)],
        axis=0,
    )
    high, low = halves(values)
    points = dot(
        jnp.concatenate([high, low, high], axis=1), thrice(tab["coarse_y"], 0)
    )
    flip = lax.broadcasted_iota(jnp.int32, (32, LOW), 1) & 1
    edge = jnp.where(flip == 0, 1.0, -1.0) * values[:, 12:13]
    high, low = halves(jnp.concatenate([points, edge], axis=0))
    share = dot(
        tab["coarse_x"], jnp.concatenate([high, low, high, jnp.zeros_like(low)], axis=0)
    )
    for odd in range(2):
        for side in range(2):
            piece = share[128 * odd : 128 * odd + 128, 128 * side : 128 * side + 128]
            piece = pltpu.roll(piece, scalars[0], 0)
            store(out_ref, 16 + 2 * odd + side, 20, piece)


def drive_blocks(rank, values):
    shape = (128, 128)
    source = row_ids()
    lane = lane_ids()
    number = 8 * (lane >> 5) + (lane & 7)
    side = jnp.where(number == 0, 0, jnp.where(number == 31, 1, 4))
    made = []
    for group in range(2):
        for q in range(4):
            slot = 4 * q + ((lane >> 3) & 3)
            back = jnp.where(slot == 0, 16 * group, 32 - slot)
            near, far = (slot, back) if group == 0 else (back, jnp.where(slot == 0, 16, slot))
            slot = jnp.where(rank < 64, near, far)
            for part in range(2):
                want = 64 * part + 32 * side + slot
                want = jnp.where(side == 4, -1, want)
                made.append(jnp.where(source == want, 1.0, 0.0).astype(jnp.bfloat16))
    select = jnp.concatenate(made, axis=1)
    high, low = halves(values)
    out = dot(
        jnp.concatenate([high, low], axis=1), jnp.concatenate([select, select], axis=0)
    )
    return lambda place: out[:, 128 * place : 128 * place + 128]


def middle_kernel(scalars, in_ref, state_ref, *rest):
    tab = Tables(MIDDLE, rest)
    ahead_ref, out_ref, next_ref = rest[len(MIDDLE) :]
    rank, cutoff = scalars[0], scalars[1]
    radii = [scalars[2 + k] for k in range(SHELLS)]
    lane = lane_ids()
    drive_of = drive_blocks(rank, load(in_ref, 16, 17))
    low0 = [0.0, 0.0]
    low1 = [0.0, 0.0]
    for group in range(2):
        real, imag = x_forward(tab, *load_set(in_ref, 8 * group, 17))
        for q in range(4):
            wave = Waves(rank, group, q)
            keep = wave.keep(cutoff)
            shell = wave.shell(radii)
            low = wave.low()
            damp = viscosity * wave.lap
            spot = 4 * group + q
            mine = (lane < 32) & ((lane & 7) == spot)
            for part, term in enumerate((real[q], imag[q])):
                place = 8 * group + 2 * q + part
                now = block(state_ref, place)
                drive = jnp.where(shell, drive_of(place), 0.0)
                slope = drive - jnp.where(keep, term, 0.0) - damp * now
                after = now + time_step * slope
                put(next_ref, place, after)
                rest_slope = slope + drive - damp * after
                done = now + 0.5 * time_step * rest_slope
                lifted = jnp.where(low, done + coarse_ratio * (done - now), done)
                put(ahead_ref, place, lifted)
                lifted = jnp.where(low, lifted, 0.0)
                low0[part] = jnp.where(mine, roll(lifted, spot), low0[part])
                low1[part] = jnp.where(mine, roll(lifted, 25 + spot), low1[part])
    even = [a + b for a, b in zip(low0, low1)]
    odd = [a - b for a, b in zip(low0, low1)]
    cos, sin = tab.turn("half", 0), tab.turn("half", 1)
    odd = [odd[0] * cos - odd[1] * sin, odd[0] * sin + odd[1] * cos]
    both = [jnp.where(lane < 32, e, roll(o, 32)) for e, o in zip(even, odd)]
    both = [jnp.where(lane < 64, b, 0.0) for b in both]
    second, first = left_many(tab["left"], [both[1]], [both[0]])
    store(out_ref, 34, 35, jnp.where(lane < 64, first[0], roll(second[0], 64)))
    state = lambda group, q: (
        block(next_ref, 8 * group + 2 * q),
        block(next_ref, 8 * group + 2 * q + 1),
    )
    send_fields(tab, rank, state, out_ref, 35, ("u", "v", "wx", "wy"))


def final_kernel(scalars, in_ref, ahead_ref, coarse_ref, *rest):
    tab = Tables(WAVES, rest)
    out_ref, points_ref = rest[len(WAVES) :]
    rank, cutoff = scalars[0], scalars[1]
    for odd in range(2):
        for side in range(2):
            total = jnp.sum(load(in_ref, 16 + 2 * odd + side, 20), axis=0, keepdims=True)
            at = slice(128 * side, 128 * side + 128)
            points_ref[odd : odd + 1, at] = coarse_ref[odd : odd + 1, at] + total
    for group in range(2):
        real, imag = x_forward(tab, *load_set(in_ref, 8 * group, 20))
        for q in range(4):
            wave = Waves(rank, group, q)
            factor = jnp.where(wave.low(), (1 + coarse_ratio) * 0.5 * time_step, 0.5 * time_step)
            factor = jnp.where(wave.keep(cutoff), factor, 0.0)
            for part, term in enumerate((real[q], imag[q])):
                lifted = block(ahead_ref, 8 * group + 2 * q + part) - factor * term
                flipped = lifted.T
                for kh in range(4):
                    for slot in range(4):
                        at = 32 * kh + 8 * slot
                        piece = flipped[at : at + 8, :]
                        number = 4 * q + slot
                        if group == 1:
                            number = 16 if number == 0 else 32 - number
                        for kl in range(8):
                            col = 128 * (8 * kh + kl)
                            out_ref[part, number, col : col + 128] = piece[kl]


VMEM = pl.BlockSpec(memory_space=pltpu.VMEM)
SMEM = pl.BlockSpec(memory_space=pltpu.SMEM)


def call(kernel, name, outs, args, scalar=False):
    specs = [SMEM] if scalar else []
    specs = specs + [VMEM] * (len(args) - len(specs))
    return pl.pallas_call(
        kernel,
        name=name,
        out_shape=[jax.ShapeDtypeStruct(shape, jnp.float32) for shape in outs],
        in_specs=specs,
        out_specs=[VMEM] * len(outs),
        compiler_params=pltpu.CompilerParams(vmem_limit_bytes=VMEM_LIMIT * 1024 * 1024),
    )(*args)


def exchange(buffer, count):
    cut = buffer.reshape(128, 1, count * 128)
    cut = lax.all_to_all(cut, AXES, split_axis=0, concat_axis=0, tiled=True)
    return cut.reshape(128 * count, 128)


@functools.lru_cache(None)
def coarse_table():
    source = np.array([0, 1, 2, 3, 124, 125, 126, 127])
    slot = np.arange(32)
    inner, spot = slot >> 3, slot & 7
    number = 4 * (spot & 3) + inner
    row = np.where(spot < 4, number, np.where(number == 0, 16, 32 - number))
    wave = 32 * source[:, None] + row[None, :]
    angle = 2 * np.pi * ((wave[:, :, None] * np.arange(LOW)) % LOW) / LOW
    return (np.stack([np.cos(angle), -np.sin(angle)], axis=1) * (8 / LOW)).astype(np.float32)


def body(vorticity_grid, forcing_grid, cutoff, forcing_shells):
    rank = lax.axis_index("gx") * lax.axis_size("gy") + lax.axis_index("gy")
    scalars = jnp.concatenate([rank[None].astype(jnp.int32), cutoff, forcing_shells])
    made = {name: jnp.asarray(table) for name, table in tables().items()}
    tabs = lambda names: tuple(made[name] for name in names)
    spectrum = (16 * 128, 128)
    (sent,) = call(
        first_kernel, "first", [(128 * 17, 128)], (vorticity_grid, forcing_grid) + tabs(FIRST)
    )
    got = exchange(sent, 17)
    state, fields = call(
        start_kernel, "start", [spectrum, (128 * 26, 128)], (scalars, got) + tabs(WAVES), True
    )
    got = exchange(fields, 26)
    (term,) = call(
        product_first_kernel, "product_first", [(128 * 17, 128)], (got, sent) + tabs(ROWS)
    )
    got = exchange(term, 17)
    ahead, fields, _ = call(
        middle_kernel,
        "middle",
        [spectrum, (128 * 35, 128), spectrum],
        (scalars, got, state) + tabs(MIDDLE),
        True,
    )
    got = exchange(fields, 35)
    term, mixed = call(
        product_kernel,
        "product",
        [(128 * 20, 128), (8, 128)],
        (scalars, got) + tabs(LAST),
        True,
    )
    got = exchange(term, 20)
    coarse = jnp.einsum(
        "sceq,scqb->eb",
        mixed.reshape(8, 2, 2, 32),
        jnp.asarray(coarse_table()),
        precision=lax.Precision.HIGHEST,
    )
    lifted, coarse = call(
        final_kernel,
        "final",
        [(2, 32, GRID), (2, LOW)],
        (scalars, got, ahead, coarse) + tabs(WAVES),
        True,
    )
    return lifted, coarse


def solution(mesh):
    placed = (P(AXES, None), P(AXES, None), P(), P())
    return jax.shard_map(
        body,
        mesh=mesh,
        in_specs=placed,
        out_specs=(P(None, AXES, None), P(AXES, None)),
        check_vma=False,
    )
```

```python
import functools
import math

import jax
import jax.numpy as jnp
import numpy as np
from jax import lax
from jax.experimental import pallas as pl
from jax.experimental.pallas import tpu as pltpu
from jax.sharding import PartitionSpec as P

GRID = 4096
LANES = 128
LOW = 256
SHELLS = 4
VMEM_LIMIT = 24
AXES = ("gx", "gy")

time_step = 0.05
viscosity = 0.05
coarse_ratio = 4.0
unit = 2.0 * math.pi / GRID


def split_np(table, axis):
    high = table.astype(np.float32).astype(jnp.bfloat16)
    low = (table - high.astype(np.float64)).astype(np.float32).astype(jnp.bfloat16)
    return np.concatenate([high, low], axis=axis)


@functools.lru_cache(None)
def tables():
    made = {}
    index = np.arange(128)
    rows = index[:, None]
    angle = 2 * np.pi * np.outer(index, index) / 128
    cos, sin = np.cos(angle) / 8, np.sin(angle) / 8
    made["left"] = split_np(np.block([[cos, sin], [-sin, cos]]), 1)

    lane = np.arange(128)
    inner = 8 * (lane >> 5) + (lane & 7)
    slot = (lane >> 3) & 3
    same = slot[:, None] == slot[None, :]
    angle = 2 * np.pi * np.outer(inner, inner) / 32
    cos, sin = same * np.cos(angle) / 8, same * np.sin(angle) / 8
    made["right_x"] = split_np(np.block([[cos, -sin], [sin, cos]]), 0)

    wide = np.arange(256)
    col_j, col_x = wide >> 3, wide & 7
    out_t, out_x = lane >> 3, lane & 7
    same = col_x[:, None] == out_x[None, :]
    angle = 2 * np.pi * np.outer(col_j, out_t) / 32
    part0 = np.cos(angle)
    part1 = -np.sin(angle)
    part1[:, out_t == 0] = np.where(col_j % 2 == 0, 1.0, -1.0)[:, None]
    right_y = np.concatenate([same * part0, same * part1], axis=1) / 8
    made["forward_y"] = split_np(right_y, 0)
    made["inverse_y"] = split_np(right_y.T, 0)

    turn = 2 * np.pi * rows * inner[None, :] / GRID
    made["turn_x"] = planes([np.cos(turn), np.sin(turn)])
    turn_d = 2 * np.pi * rows * out_t[None, :] / GRID
    back = np.where(out_t == 0, 16, 32 - out_t)
    turn_m = 2 * np.pi * rows * back[None, :] / GRID
    made["turn_y"] = planes([np.cos(turn_d), np.sin(turn_d), np.cos(turn_m), np.sin(turn_m)])
    half = 2 * np.pi * rows / 256 + np.zeros((128, 128))
    made["half"] = planes([np.cos(half), np.sin(half)])

    column = rows + 128 * inner[None, :]
    mx = np.where(column < GRID // 2, column, column - GRID)
    made["wave_x"] = planes(
        [
            np.where(column == GRID // 2, 0, mx) * unit,
            mx * mx,
            np.where((mx >= -LOW // 2) & (mx < LOW // 2), 1.0, 0.0),
        ]
    )

    spot = np.arange(32)
    inside, group, quarter = spot >> 3, (spot >> 2) & 1, spot & 3
    number = 4 * quarter + inside
    number = np.where(group == 0, number, np.where(number == 0, 16, 32 - number))
    made["drive_spots"] = np.concatenate(
        [
            np.kron(np.eye(4), index[:32, None] == want[None, :])
            for want in (number, (32 - number) % 32)
        ],
        axis=0,
    ).astype(jnp.bfloat16)

    point = np.arange(LOW)[None, :]
    angle = 2 * np.pi * (np.tile(number, 4)[:, None] * point % LOW) / LOW
    plain = ((lane >> 5) & 1 == 0)[:, None] * (8 / LOW)
    imag = (lane >= 64)[:, None]
    made["coarse_rows"] = split_np(
        np.concatenate(
            [
                plain * np.where(imag, -np.sin(angle), np.cos(angle)),
                plain * np.where(imag, np.cos(angle), np.sin(angle)),
            ],
            axis=1,
        ),
        0,
    )
    source = np.array([0, 1, 2, 3, 124, 125, 126, 127])[:, None]
    angle = 2 * np.pi * (source * point % 8) / 8
    made["coarse_turn"] = planes([np.cos(angle), -np.sin(angle)])

    angle = 2 * np.pi * np.outer(index, index) / GRID
    low = np.concatenate([np.cos(angle), -np.sin(angle)], axis=0) / 64
    made["low_rows"] = split_np(low, 1)
    turn = 2 * np.pi * rows * out_t[None, :] / 32
    made["turn_low"] = planes([np.cos(turn), np.sin(turn)])

    grid = np.arange(512)
    t, group, part, source = grid >> 5, (grid >> 4) & 1, (grid >> 3) & 1, grid & 7
    number = np.where(group == 0, t, np.where(t == 0, 16, 32 - t))
    wave = 32 * source + number
    point = np.arange(LOW)[None, :]
    angle = 2 * np.pi * (wave[:, None] * point % LOW) / LOW
    weight = np.where(wave == 0, 1.0, np.where(wave < 128, 2.0, 0.0))
    weight = np.where((wave == 128) & (part == 0), 1.0, weight)
    value = np.where(part[:, None] == 0, np.cos(angle), -np.sin(angle))
    made["coarse_y"] = split_np(weight[:, None] * value, 0)
    away = np.arange(128)[:, None]
    own = np.arange(32)[None, :]
    parts = []
    for odd in range(2):
        place = 32 * away + 16 * odd - own
        kernel = 1.0 + 2.0 * sum(
            np.cos(2 * np.pi * (p * place % GRID) / GRID) for p in range(1, 128)
        )
        sign = 1.0 - 2.0 * odd
        edge = 2 * np.pi * own / 32 + 0 * away
        parts.append(
            np.concatenate([kernel + sign * np.cos(edge), sign * np.sin(edge)], axis=1)
        )
    scale = -(1 + coarse_ratio) * 0.5 * time_step / (64 * LOW)
    both = np.concatenate(parts, axis=0) * scale
    both = split_np(both, 1)
    high, low = both[:, :64], both[:, 64:]
    made["coarse_x"] = np.concatenate([high, high, low, 0 * low], axis=1)
    return made


def planes(parts):
    return np.concatenate(parts, axis=0).astype(np.float32)


def halves(values):
    high = values.astype(jnp.bfloat16)
    low = (values - high.astype(jnp.float32)).astype(jnp.bfloat16)
    return high, low


def dot(left_side, right_side):
    return jnp.dot(left_side, right_side, preferred_element_type=jnp.float32)


def thrice(table, axis):
    size = table.shape[axis] // 2
    high = lax.slice_in_dim(table, 0, size, axis=axis)
    low = lax.slice_in_dim(table, size, 2 * size, axis=axis)
    return jnp.concatenate([high, high, low], axis=axis)


def left_many(left_table, real, imag):
    count = len(real)
    stacked = jnp.concatenate(
        [jnp.concatenate(real, axis=1), jnp.concatenate(imag, axis=1)], axis=0
    )
    high, low = halves(stacked)
    out = dot(thrice(left_table, 1), jnp.concatenate([high, low, high], axis=0))
    cut = lambda row, place: out[row : row + 128, 128 * place : 128 * place + 128]
    return [cut(0, k) for k in range(count)], [cut(128, k) for k in range(count)]


def right_many(right_table, first, second):
    count = len(first)
    stacked = jnp.concatenate(
        [jnp.concatenate([a, b], axis=1) for a, b in zip(first, second)], axis=0
    )
    high, low = halves(stacked)
    out = dot(jnp.concatenate([high, low, high], axis=1), thrice(right_table, 0))
    cut = lambda row, col: out[128 * row : 128 * row + 128, col : col + 128]
    return [cut(k, 0) for k in range(count)], [cut(k, 128) for k in range(count)]


def lane_ids():
    return lax.broadcasted_iota(jnp.int32, (128, 128), 1)


def row_ids():
    return lax.broadcasted_iota(jnp.int32, (128, 128), 0)


def roll(block, shift):
    shift = shift % 128
    return block if shift == 0 else pltpu.roll(block, shift, 1)


def swap4(blocks):
    lane = lax.broadcasted_iota(jnp.int32, blocks[0].shape, 1)
    out = list(blocks)
    for bit, shift in ((0, 32), (1, 64)):
        low = ((lane >> (5 + bit)) & 1) == 0
        made = list(out)
        for index in range(4):
            if (index >> bit) & 1 == 0:
                a, b = out[index], out[index | (1 << bit)]
                made[index] = jnp.where(low, a, roll(b, shift))
                made[index | (1 << bit)] = jnp.where(low, roll(a, -shift), b)
        out = made
    return out


def turned(real, imag, cos, sin):
    return real * cos + imag * sin, imag * cos - real * sin


class Tables:
    def __init__(self, names, refs):
        self.refs = dict(zip(names, refs))

    def __getitem__(self, name):
        return self.refs[name][...]

    def turn(self, name, index):
        return self.refs[name][128 * index : 128 * index + 128, :]


def x_turned(tab, first, second):
    cos, sin = tab.turn("turn_x", 0), tab.turn("turn_x", 1)
    pairs = [turned(a, b, cos, sin) for a, b in zip(first, second)]
    return [p[0] for p in pairs], [p[1] for p in pairs]


def x_plain(tab, real, imag):
    real, imag = left_many(tab["left"], real, imag)
    return right_many(tab["right_x"], *x_turned(tab, real, imag))


def x_forward(tab, real, imag):
    return x_plain(tab, swap4(real), swap4(imag))


def x_inverse(tab, real, imag):
    first, second = right_many(tab["right_x"], imag, real)
    first, second = left_many(tab["left"], *x_turned(tab, first, second))
    return second, first


def y_forward(tab, groups):
    part0, part1 = right_many(
        tab["forward_y"], [g[0] for g in groups], [g[1] for g in groups]
    )
    start = lane_ids() < 8
    cos, sin = tab.turn("turn_y", 0), tab.turn("turn_y", 1)
    rest = jnp.where(start, 0.0, cos)
    real = [p * cos + q * sin for p, q in zip(part0, part1)]
    imag = [q * rest - p * sin for p, q in zip(part0, part1)]
    direct = left_many(tab["left"], real, imag)
    cos, sin = tab.turn("turn_y", 2), tab.turn("turn_y", 3)
    a, b = jnp.where(start, 0.0, cos), jnp.where(start, cos, -sin)
    d, e = jnp.where(start, 0.0, -sin), jnp.where(start, -sin, -cos)
    real = [p * a + q * b for p, q in zip(part0, part1)]
    imag = [p * d + q * e for p, q in zip(part0, part1)]
    mirror = left_many(tab["left"], real, imag)
    return direct, mirror


def y_inverse(tab, real, imag, last, place):
    imag, real = left_many(tab["left"], imag, real)
    start = lane_ids() < 8
    cos, sin = tab.turn("turn_y", 0), tab.turn("turn_y", 1)
    cos = jnp.where(start, cos, 2.0 * cos)
    sin = 2.0 * sin
    part0 = [p * cos - q * sin for p, q in zip(real, imag)]
    part1 = [p * sin + q * cos for p, q in zip(real, imag)]
    part1 = [
        jnp.where(start, roll(last, -(32 * xh + 8 * place)), part1[xh]) for xh in range(4)
    ]
    return right_many(tab["inverse_y"], part0, part1)


def last_row(tab, real, imag):
    imag, real = left_many(tab["left"], [imag], [real])
    return real[0] * tab.turn("half", 0) - imag[0] * tab.turn("half", 1)


def load(ref, index, count):
    return ref[pl.ds(index, 128, stride=count), :]


def store(ref, index, count, block):
    ref[pl.ds(index, 128, stride=count), :] = block


def load_set(ref, base, count):
    real = [load(ref, base + k, count) for k in range(4)]
    imag = [load(ref, base + 4 + k, count) for k in range(4)]
    return real, imag


def store_set(ref, base, count, real, imag):
    for k in range(4):
        store(ref, base + k, count, real[k])
        store(ref, base + 4 + k, count, imag[k])


def block(ref, index):
    return ref[128 * index : 128 * index + 128, :]


def put(ref, index, value):
    ref[128 * index : 128 * index + 128, :] = value


def rank_here():
    return lax.axis_index("gx") * lax.axis_size("gy") + lax.axis_index("gy")


class Rows:
    def __init__(self, rank, group, quarter):
        lane = lax.broadcasted_iota(jnp.int32, (1, 128), 1)
        slot = 4 * quarter + ((lane >> 3) & 3)
        if group == 1:
            slot = jnp.where(slot == 0, 16, 32 - slot)
        row = 32 * rank + slot
        my = jnp.where(row < GRID // 2, row, row - GRID)
        self.my = my
        self.square = (my * my).astype(jnp.float32)
        self.slope = jnp.where(row == GRID // 2, 0, my).astype(jnp.float32) * unit

    def keep(self, cutoff):
        return jnp.where(jnp.abs(self.my) <= cutoff, 1.0, 0.0)

    def low(self):
        half = LOW // 2
        return jnp.where((self.my >= -half) & (self.my < half), 1.0, 0.0)


def keep_columns(tab, cutoff):
    return jnp.where(tab.turn("wave_x", 1) <= (cutoff * cutoff).astype(jnp.float32), 1.0, 0.0)


def send_fields(tab, rank, state, out_ref, count, names, extra=None):
    total = len(names)
    last_real, last_imag = None, None
    lane_slot = (lane_ids() >> 3) & 3
    rows = [Rows(rank, 0, q) for q in range(4)] + [Rows(rank, 1, 0)]
    across, squares = tab.turn("wave_x", 0), tab.turn("wave_x", 1)
    sources = {}
    for index in range(5):
        real, imag = state(0, index) if index < 4 else state(1, 0)
        both = squares + rows[index].square
        scale = jnp.where(both == 0.0, 0.0, (1.0 / (unit * unit)) / jnp.maximum(both, 1.0))
        sources["w", index] = real, imag
        sources["psi", index] = real * scale, imag * scale
    for place, name in enumerate(names):
        reals, imags = [], []
        for index in range(5):
            real, imag = sources["psi" if name in ("u", "v") else "w", index]
            factor = rows[index].slope if name in ("u", "wy") else across
            if name == "v":
                reals.append(imag * factor)
                imags.append(-real * factor)
            else:
                reals.append(-imag * factor)
                imags.append(real * factor)
        mine = lane_slot == place
        moved = roll(reals[4], 8 * place), roll(imags[4], 8 * place)
        last_real = jnp.where(mine, moved[0], 0.0 if last_real is None else last_real)
        last_imag = jnp.where(mine, moved[1], 0.0 if last_imag is None else last_imag)
        real, imag = x_inverse(tab, reals[:4], imags[:4])
        store_set(out_ref, 8 * place, count, swap4(real), swap4(imag))
    real, imag = x_inverse(tab, [last_real], [last_imag])
    real, imag = real[0], imag[0]
    if extra is not None:
        real, imag = extra(real, 0), extra(imag, 1)
    store(out_ref, 8 * total, count, real)
    store(out_ref, 8 * total + 1, count, imag)


FIRST = ("left", "forward_y", "turn_y", "low_rows", "turn_low")
WAVES = ("left", "right_x", "turn_x", "wave_x")
MIDDLE = WAVES + ("half",)
FINAL = WAVES + ("coarse_rows", "coarse_turn")
ROWS = ("left", "forward_y", "inverse_y", "turn_y", "half")
PRODUCT = ROWS + ("drive_spots",)
LAST = ROWS + ("coarse_y", "coarse_x")


def grid_groups(ref):
    groups = []
    for xh in range(4):
        pair = []
        for jh in range(2):
            pieces = [
                ref[8 * xh : 8 * xh + 8, 128 * j : 128 * j + 128]
                for j in range(16 * jh, 16 * jh + 16)
            ]
            pair.append(jnp.concatenate(pieces, axis=0).T)
        groups.append(pair)
    return groups


def first_kernel(*rest):
    total = 2 + len(FIRST)
    out_ref, *held, ready = rest[total + 1 :]
    copies = {}
    for name in ("rows", "forward_y", "turn_y", "left", "force", "low_rows", "turn_low"):
        k = ("rows", "force").index(name) if name in ("rows", "force") else 2 + FIRST.index(name)
        copies[name] = pltpu.make_async_copy(rest[k], held[k], ready.at[k])
        copies[name].start()
    vorticity_ref, forcing_ref = held[:2]
    tab = Tables(FIRST, held[2:])
    for name in ("rows", "forward_y", "turn_y", "left"):
        copies[name].wait()
    direct, mirror = y_forward(tab, grid_groups(vorticity_ref))
    store_set(out_ref, 0, 17, *direct)
    store_set(out_ref, 8, 17, *mirror)
    for name in ("force", "low_rows", "turn_low"):
        copies[name].wait()
    groups = grid_groups(forcing_ref)
    values = jnp.concatenate([g[k] for g in groups for k in range(2)], axis=1)
    high, low = halves(values)
    out = dot(thrice(tab["low_rows"], 1), jnp.concatenate([high, low, high], axis=0))
    lane, row = lane_ids(), row_ids()
    sign = jnp.where((row & 1) == 0, 1.0, -1.0)
    cos, sin = tab.turn("turn_low", 0), tab.turn("turn_low", 1)
    packed = jnp.zeros((128, 128), jnp.float32)
    for xh in range(4):
        at = 256 * xh
        real = out[:128, at : at + 128] + sign * out[:128, at + 128 : at + 256]
        imag = out[128:, at : at + 128] + sign * out[128:, at + 128 : at + 256]
        for part, value in enumerate(turned(real, imag, cos, sin)):
            for shift in (64, 32, 16, 8):
                value = value + roll(value, shift)
            mine = ((lane >> 5) == xh) & (((lane >> 3) & 3) == part)
            packed = jnp.where(mine, value, packed)
    store(out_ref, 16, 17, packed)


def start_kernel(in_ref, *rest):
    tab = Tables(WAVES, rest)
    state_ref, out_ref = rest[len(WAVES) :]
    rank = rank_here()
    for group in range(2):
        real, imag = x_forward(tab, *load_set(in_ref, 8 * group, 17))
        for q in range(4):
            put(state_ref, 8 * group + 2 * q, real[q])
            put(state_ref, 8 * group + 2 * q + 1, imag[q])
    row = load(in_ref, 16, 17)
    lane = lane_ids()
    part = (lane >> 3) & 3
    real = jnp.where(part == 0, row, jnp.where(part == 1, roll(row, 8), 0.0))
    imag = jnp.where(part == 0, roll(row, -8), jnp.where(part == 1, -row, 0.0))
    real, imag = x_plain(tab, [real], [imag])

    def extra(values, which):
        source = (real, imag)[which][0]
        for spot, origin in enumerate((0, 103, 8, 111)):
            moved = roll(source, 24 + spot - origin)
            values = jnp.where(lane == 24 + spot, moved, values)
        return values

    state = lambda group, q: (
        block(state_ref, 8 * group + 2 * q),
        block(state_ref, 8 * group + 2 * q + 1),
    )
    send_fields(tab, rank, state, out_ref, 26, ("u", "v", "wx"), extra)


def product_one(tab, in_ref, count, last, place):
    real, imag = load_set(in_ref, 8 * place, count)
    return y_inverse(tab, real, imag, last, place)


def drive_rows(tab, real, imag):
    lane = lane_ids()
    columns = jnp.where(lane < 4, roll(real, -24), roll(imag, -20)).T
    pick = lambda index: jnp.broadcast_to(columns[index : index + 1, :], (8, 128))
    plus = swap4([pick(4 * part + k) for part in range(2) for k in range(2)])
    minus = swap4([pick(4 * part + 2 + k) for part in range(2) for k in range(2)])
    sub = lax.broadcasted_iota(jnp.int32, (8, 128), 0)
    start = (lax.broadcasted_iota(jnp.int32, (8, 128), 1) & 31) == 0
    top = jnp.zeros((8, 128), jnp.float32)
    bottom = jnp.zeros((8, 128), jnp.float32)
    for k in range(4):
        top = jnp.where(sub == k, plus[k], top)
        after = minus[k + 1] if k < 3 else 0.0
        bottom = jnp.where(sub == 7 - k, jnp.where(start, after, minus[k]), bottom)
    spots = tab["drive_spots"]
    made = []
    for values, table in ((top, spots[:128]), (bottom, spots[128:])):
        high, low = halves(values)
        made.append(dot(high, table) + dot(low, table))
    return jnp.concatenate([made[0], jnp.zeros((112, 128), jnp.float32), made[1]], axis=0)


def product_first_kernel(in_ref, local_ref, *rest):
    tab = Tables(PRODUCT, rest)
    out_ref = rest[len(PRODUCT)]
    last_real, last_imag = load(in_ref, 24, 26), load(in_ref, 25, 26)
    store(out_ref, 16, 17, drive_rows(tab, last_real, last_imag))
    last = last_row(tab, last_real, last_imag)
    u0, u1 = product_one(tab, in_ref, 26, last, 0)
    x0, x1 = product_one(tab, in_ref, 26, last, 2)
    sum0 = [a * b for a, b in zip(u0, x0)]
    sum1 = [a * b for a, b in zip(u1, x1)]
    lane = lane_ids()
    row = 32 * row_ids() + (lane >> 3)
    slope = jnp.where(row < GRID // 2, row, row - GRID)
    slope = jnp.where(row == GRID // 2, 0, slope).astype(jnp.float32) * unit
    real, imag = load_set(local_ref, 0, 17)
    real, imag = [-b * slope for b in imag], [a * slope for a in real]
    row = 32 * row_ids() + 16
    slope = jnp.where(row < GRID // 2, row, row - GRID).astype(jnp.float32) * unit
    last_real, last_imag = 0.0, 0.0
    for xh in range(4):
        mine = (lane >> 3) == 4 * xh
        a, b = load(local_ref, 8 + xh, 17), load(local_ref, 12 + xh, 17)
        last_real = jnp.where(mine, roll(-b * slope, 32 * xh), last_real)
        last_imag = jnp.where(mine, roll(a * slope, 32 * xh), last_imag)
    own = last_row(tab, last_real, last_imag)
    y0, y1 = y_inverse(tab, real, imag, own, 0)
    v0, v1 = product_one(tab, in_ref, 26, last, 1)
    sum0 = [s + a * b for s, a, b in zip(sum0, v0, y0)]
    sum1 = [s + a * b for s, a, b in zip(sum1, v1, y1)]
    direct, mirror = y_forward(tab, list(zip(sum0, sum1)))
    store_set(out_ref, 0, 17, *direct)
    store_set(out_ref, 8, 17, *mirror)


def product_kernel(in_ref, *rest):
    tab = Tables(LAST, rest)
    out_ref, mixed_ref = rest[len(LAST) :]
    got = load(in_ref, 34, 35)
    mixed_ref[0:4, :] = got[0:4, :]
    mixed_ref[4:8, :] = got[124:128, :]
    last = last_row(tab, load(in_ref, 32, 35), load(in_ref, 33, 35))
    sum0, sum1 = None, None
    for one, two in ((0, 2), (1, 3)):
        a0, a1 = product_one(tab, in_ref, 35, last, one)
        b0, b1 = product_one(tab, in_ref, 35, last, two)
        made0 = [a * b for a, b in zip(a0, b0)]
        made1 = [a * b for a, b in zip(a1, b1)]
        sum0 = made0 if sum0 is None else [s + m for s, m in zip(sum0, made0)]
        sum1 = made1 if sum1 is None else [s + m for s, m in zip(sum1, made1)]
    direct, mirror = y_forward(tab, list(zip(sum0, sum1)))
    store_set(out_ref, 0, 20, *direct)
    store_set(out_ref, 8, 20, *mirror)
    pieces = []
    for xh in range(4):
        for part in (direct[0], direct[1], mirror[0], mirror[1]):
            pieces.append(part[xh][0:8, :])
    across = jnp.concatenate(pieces, axis=0).T
    made = [
        swap4([across[8 * t : 8 * t + 8, :] for t in range(4 * tq, 4 * tq + 4)])
        for tq in range(4)
    ]
    values = jnp.concatenate(
        [jnp.concatenate([made[tq][xh] for tq in range(4)], axis=1) for xh in range(4)],
        axis=0,
    )
    high, low = halves(values)
    points = dot(
        jnp.concatenate([high, low, high], axis=1), thrice(tab["coarse_y"], 0)
    )
    flip = lax.broadcasted_iota(jnp.int32, (32, LOW), 1) & 1
    edge = jnp.where(flip == 0, 1.0, -1.0) * values[:, 12:13]
    high, low = halves(jnp.concatenate([points, edge], axis=0))
    share = dot(
        tab["coarse_x"], jnp.concatenate([high, low, high, jnp.zeros_like(low)], axis=0)
    )
    for odd in range(2):
        for side in range(2):
            piece = share[128 * odd : 128 * odd + 128, 128 * side : 128 * side + 128]
            piece = pltpu.roll(piece, rank_here(), 0)
            store(out_ref, 16 + 2 * odd + side, 20, piece)


def shelled(rank, values, radii):
    lane = lane_ids()
    side, spot = (lane >> 5) & 1, lane & 7
    slot = 4 * (spot & 3) + ((lane >> 3) & 3)
    slot = jnp.where(spot < 4, slot, jnp.where(slot == 0, 16, 32 - slot))
    my = 32 * rank + slot
    my = jnp.where(my < GRID // 2, my, my - GRID)
    mx = row_ids() - 128 * side
    squares = mx * mx + my * my
    mask = None
    for radius in radii:
        inside = (radius * radius <= squares) & (squares < (radius + 1) * (radius + 1))
        mask = inside if mask is None else mask | inside
    return jnp.where(mask, values, 0.0)


def fetch(ready, pairs):
    copies = [
        pltpu.make_async_copy(source, target, ready.at[k])
        for k, (source, target) in enumerate(pairs)
    ]
    for copy in copies:
        copy.start()
    return copies


def middle_kernel(cutoff_from, shells_from, in_ref, state_ref, *rest):
    tab = Tables(MIDDLE, rest)
    ahead_ref, out_ref, next_ref, cutoff_ref, shells_ref, ready = rest[len(MIDDLE) :]
    copies = fetch(ready, ((cutoff_from, cutoff_ref), (shells_from, shells_ref)))
    rank = rank_here()
    lane = lane_ids()
    spectra = [x_forward(tab, *load_set(in_ref, 8 * group, 17)) for group in range(2)]
    for copy in copies:
        copy.wait()
    cutoff = cutoff_ref[0]
    forcing = shelled(rank, load(in_ref, 16, 17), [shells_ref[k] for k in range(SHELLS)])
    first_spots = (lane < 32) & ((lane & 7) == 0)
    last_spots = (lane >= 96) & ((lane & 7) == 7)
    keep_x = keep_columns(tab, cutoff)
    squares, low_x = tab.turn("wave_x", 1), tab.turn("wave_x", 2)
    low0 = [0.0, 0.0]
    low1 = [0.0, 0.0]
    for group in range(2):
        real, imag = spectra[group]
        for q in range(4):
            rows = Rows(rank, group, q)
            keep = keep_x * rows.keep(cutoff)
            low = low_x * rows.low()
            damp = (viscosity * unit * unit) * (squares + rows.square)
            spot = 4 * group + q
            mine = (lane < 32) & ((lane & 7) == spot)
            for part, term in enumerate((real[q], imag[q])):
                place = 8 * group + 2 * q + part
                now = block(state_ref, place)
                drive = jnp.where(first_spots, roll(forcing, -64 * part - spot), 0.0)
                drive = jnp.where(
                    last_spots, roll(forcing, 71 - 64 * part - spot), drive
                )
                slope = drive - keep * term - damp * now
                after = now + time_step * slope
                put(next_ref, place, after)
                rest_slope = slope + drive - damp * after
                change = 0.5 * time_step * rest_slope
                lifted = now + change + (coarse_ratio * low) * change
                put(ahead_ref, place, lifted)
                lifted = low * lifted
                low0[part] = jnp.where(mine, roll(lifted, spot), low0[part])
                low1[part] = jnp.where(mine, roll(lifted, 25 + spot), low1[part])
    even = [a + b for a, b in zip(low0, low1)]
    odd = [a - b for a, b in zip(low0, low1)]
    cos, sin = tab.turn("half", 0), tab.turn("half", 1)
    odd = [odd[0] * cos - odd[1] * sin, odd[0] * sin + odd[1] * cos]
    both = [jnp.where(lane < 32, e, roll(o, 32)) for e, o in zip(even, odd)]
    both = [jnp.where(lane < 64, b, 0.0) for b in both]
    second, first = left_many(tab["left"], [both[1]], [both[0]])
    store(out_ref, 34, 35, jnp.where(lane < 64, first[0], roll(second[0], 64)))
    state = lambda group, q: (
        block(next_ref, 8 * group + 2 * q),
        block(next_ref, 8 * group + 2 * q + 1),
    )
    send_fields(tab, rank, state, out_ref, 35, ("u", "v", "wx", "wy"))


def final_kernel(cutoff_from, in_ref, ahead_ref, mixed_ref, *rest):
    tab = Tables(FINAL, rest)
    out_ref, points_ref, held_ref, cutoff_ref, ready, done_ref = rest[len(FINAL) :]
    (copy,) = fetch(ready, ((cutoff_from, cutoff_ref),))
    rank = rank_here()
    spectra = [x_forward(tab, *load_set(in_ref, 8 * group, 20)) for group in range(2)]
    copy.wait()
    cutoff = cutoff_ref[0]
    keep_x = keep_columns(tab, cutoff) * (0.5 * time_step)
    low_x = tab.turn("wave_x", 2) * coarse_ratio
    copies = []
    for group in range(2):
        real, imag = spectra[group]
        for q in range(4):
            rows = Rows(rank, group, q)
            factor = keep_x * rows.keep(cutoff)
            factor = factor + factor * (low_x * rows.low())
            for part, term in enumerate((real[q], imag[q])):
                lifted = block(ahead_ref, 8 * group + 2 * q + part) - factor * term
                flipped = lifted.T
                for kh in range(4):
                    for slot in range(4):
                        at = 32 * kh + 8 * slot
                        piece = flipped[at : at + 8, :]
                        number = 4 * q + slot
                        if group == 1:
                            number = 16 if number == 0 else 32 - number
                        for kl in range(8):
                            col = 128 * (8 * kh + kl)
                            held_ref[part, number, col : col + 128] = piece[kl]
        for part in range(2):
            spot = (part, slice(16 * group, 16 * group + 16))
            copies.append(
                pltpu.make_async_copy(
                    held_ref.at[spot], out_ref.at[spot], done_ref.at[2 * group + part]
                )
            )
            copies[-1].start()
    mixed = mixed_ref[...]
    high, low = halves(jnp.concatenate([mixed, roll(mixed, -32)], axis=0))
    out = dot(
        jnp.concatenate([high, low, high], axis=1), thrice(tab["coarse_rows"], 0)
    )
    turn = tab["coarse_turn"]
    for odd in range(2):
        rows = out[8 * odd : 8 * odd + 8]
        rows = rows[:, :LOW] * turn[:8] + rows[:, LOW:] * turn[8:]
        line = jnp.sum(rows, axis=0, keepdims=True)
        for side in range(2):
            total = jnp.sum(load(in_ref, 16 + 2 * odd + side, 20), axis=0, keepdims=True)
            at = slice(128 * side, 128 * side + 128)
            points_ref[odd : odd + 1, at] = line[:, at] + total
    for copy in copies:
        copy.wait()


VMEM = pl.BlockSpec(memory_space=pltpu.VMEM)


HBM = pl.BlockSpec(memory_space=pltpu.HBM)


def call(kernel, name, outs, args, far=(), out_specs=None, scratch=()):
    far = tuple(
        a if a.ndim == 1 else pltpu.with_memory_space_constraint(a, pltpu.HBM) for a in far
    )
    return pl.pallas_call(
        kernel,
        name=name,
        out_shape=[jax.ShapeDtypeStruct(shape, jnp.float32) for shape in outs],
        in_specs=[HBM] * len(far) + [VMEM] * len(args),
        out_specs=out_specs or [VMEM] * len(outs),
        scratch_shapes=list(scratch),
        compiler_params=pltpu.CompilerParams(vmem_limit_bytes=VMEM_LIMIT * 1024 * 1024),
    )(*far, *args)


def near(array):
    return pltpu.with_memory_space_constraint(array, pltpu.VMEM)


def exchange(buffer, count):
    cut = buffer.reshape(128, 1, count * 128)
    cut = lax.all_to_all(cut, AXES, split_axis=0, concat_axis=0, tiled=True)
    return cut.reshape(128 * count, 128)


def body(vorticity_grid, forcing_grid, cutoff, forcing_shells):
    made = {name: jnp.asarray(table) for name, table in tables().items()}
    tabs = lambda names: tuple(made[name] for name in names)
    spectrum = (16 * 128, 128)
    args = (vorticity_grid, forcing_grid) + tabs(FIRST)
    (sent,) = call(
        first_kernel,
        "first",
        [(128 * 17, 128)],
        (),
        args + (cutoff,),
        scratch=[pltpu.VMEM(a.shape, a.dtype) for a in args]
        + [pltpu.SemaphoreType.DMA((len(args),))],
    )
    got = exchange(sent, 17)
    state, fields = call(
        start_kernel, "start", [spectrum, (128 * 26, 128)], (got,) + tabs(WAVES)
    )
    got = exchange(fields, 26)
    (term,) = call(
        product_first_kernel, "product_first", [(128 * 17, 128)], (got, near(sent)) + tabs(PRODUCT)
    )
    got = exchange(term, 17)
    ahead, fields = call(
        middle_kernel,
        "middle",
        [spectrum, (128 * 35, 128)],
        (got, near(state)) + tabs(MIDDLE),
        (cutoff, forcing_shells),
        scratch=[
            pltpu.VMEM(spectrum, jnp.float32),
            pltpu.SMEM((1,), jnp.int32),
            pltpu.SMEM((SHELLS,), jnp.int32),
            pltpu.SemaphoreType.DMA((2,)),
        ],
    )
    got = exchange(fields, 35)
    term, mixed = call(
        product_kernel, "product", [(128 * 20, 128), (8, 128)], (got,) + tabs(LAST)
    )
    got = exchange(term, 20)
    lifted, coarse = call(
        final_kernel,
        "final",
        [(2, 32, GRID), (2, LOW)],
        (got, near(ahead), mixed) + tabs(FINAL),
        (cutoff,),
        out_specs=[HBM, VMEM],
        scratch=[
            pltpu.VMEM((2, 32, GRID), jnp.float32),
            pltpu.SMEM((1,), jnp.int32),
            pltpu.SemaphoreType.DMA((1,)),
            pltpu.SemaphoreType.DMA((4,)),
        ],
    )
    return lifted, coarse


def solution(mesh):
    placed = (P(AXES, None), P(AXES, None), P(), P())
    return jax.shard_map(
        body,
        mesh=mesh,
        in_specs=placed,
        out_specs=(P(None, AXES, None), P(AXES, None)),
        check_vma=False,
    )
```

```python
import functools
import math

import jax
import jax.numpy as jnp
import numpy as np
from jax import lax
from jax.experimental import pallas as pl
from jax.experimental.pallas import tpu as pltpu
from jax.sharding import PartitionSpec as P

GRID = 4096
LANES = 128
LOW = 256
SHELLS = 4
VMEM_LIMIT = 24
AXES = ("gx", "gy")

time_step = 0.05
viscosity = 0.05
coarse_ratio = 4.0
unit = 2.0 * math.pi / GRID


def split_np(table, axis):
    high = table.astype(np.float32).astype(jnp.bfloat16)
    low = (table - high.astype(np.float64)).astype(np.float32).astype(jnp.bfloat16)
    return np.concatenate([high, low], axis=axis)


@functools.lru_cache(None)
def tables():
    made = {}
    index = np.arange(128)
    rows = index[:, None]
    angle = 2 * np.pi * np.outer(index, index) / 128
    cos, sin = np.cos(angle) / 8, np.sin(angle) / 8
    made["left"] = split_np(np.block([[cos, sin], [-sin, cos]]), 1)

    near = (index >= 1) & (index < 64)
    far = index >= 64
    angle = 2 * np.pi * np.outer(index, index) / 128
    later = 2 * np.pi * np.outer(index, index + 0.5) / 128
    real = np.where(near, 2 * np.cos(angle), np.where(index == 0, 1.0, 0.0))
    imag = np.where(near, -2 * np.sin(angle), np.where(index == 0, (-1.0) ** rows, 0.0))
    edge = [[real, imag], [far * 2 * np.cos(later), far * -2 * np.sin(later)]]
    made["left_edge"] = split_np(np.block(edge) / 8, 1)

    lane = np.arange(128)
    inner = 8 * (lane >> 5) + (lane & 7)
    slot = (lane >> 3) & 3
    same = slot[:, None] == slot[None, :]
    angle = 2 * np.pi * np.outer(inner, inner) / 32
    cos, sin = same * np.cos(angle) / 8, same * np.sin(angle) / 8
    made["right_x"] = split_np(np.block([[cos, -sin], [sin, cos]]), 0)

    wide = np.arange(256)
    col_j, col_x = wide >> 3, wide & 7
    out_t, out_x = lane >> 3, lane & 7
    same = col_x[:, None] == out_x[None, :]
    angle = 2 * np.pi * np.outer(col_j, out_t) / 32
    part0 = np.cos(angle)
    part1 = -np.sin(angle)
    part1[:, out_t == 0] = np.where(col_j % 2 == 0, 1.0, -1.0)[:, None]
    right_y = np.concatenate([same * part0, same * part1], axis=1) / 8
    made["forward_y"] = split_np(right_y, 0)
    made["inverse_y"] = split_np(right_y.T, 0)

    turn = 2 * np.pi * rows * inner[None, :] / GRID
    made["turn_x"] = planes([np.cos(turn), np.sin(turn)])
    turn_d = 2 * np.pi * rows * out_t[None, :] / GRID
    back = np.where(out_t == 0, 16, 32 - out_t)
    turn_m = 2 * np.pi * rows * back[None, :] / GRID
    made["turn_y"] = planes([np.cos(turn_d), np.sin(turn_d), np.cos(turn_m), np.sin(turn_m)])
    half = 2 * np.pi * rows / 256 + np.zeros((128, 128))
    made["half"] = planes([np.cos(half), np.sin(half)])

    column = rows + 128 * inner[None, :]
    mx = np.where(column < GRID // 2, column, column - GRID)
    made["wave_x"] = planes(
        [
            np.where(column == GRID // 2, 0, mx) * unit,
            mx * mx,
            np.where((mx >= -LOW // 2) & (mx < LOW // 2), 1.0, 0.0),
        ]
    )

    spot = np.arange(32)
    inside, group, quarter = spot >> 3, (spot >> 2) & 1, spot & 3
    number = 4 * quarter + inside
    number = np.where(group == 0, number, np.where(number == 0, 16, 32 - number))
    made["drive_spots"] = np.concatenate(
        [
            np.kron(np.eye(4), index[:32, None] == want[None, :])
            for want in (number, (32 - number) % 32)
        ],
        axis=0,
    ).astype(jnp.bfloat16)

    point = np.arange(LOW)[None, :]
    angle = 2 * np.pi * (np.tile(number, 4)[:, None] * point % LOW) / LOW
    plain = ((lane >> 5) & 1 == 0)[:, None] * (8 / LOW)
    imag = (lane >= 64)[:, None]
    made["coarse_rows"] = split_np(
        np.concatenate(
            [
                plain * np.where(imag, -np.sin(angle), np.cos(angle)),
                plain * np.where(imag, np.cos(angle), np.sin(angle)),
            ],
            axis=1,
        ),
        0,
    )
    source = np.array([0, 1, 2, 3, 124, 125, 126, 127])[:, None]
    angle = 2 * np.pi * (source * point % 8) / 8
    made["coarse_turn"] = planes([np.cos(angle), -np.sin(angle)])

    flips = [
        (slot[:, None] == slot[None, :]) & (inner[:, None] == want[None, :])
        for want in (31 - inner, (32 - inner) % 32)
    ]
    flips.append(rows == (128 - index[None, :]) % 128)
    made["flip"] = np.concatenate(flips, axis=0).astype(np.float32).astype(jnp.bfloat16)

    angle = 2 * np.pi * np.outer(index, index) / GRID
    low = np.concatenate([np.cos(angle), -np.sin(angle)], axis=0) / 64
    made["low_rows"] = split_np(low, 1)
    turn = 2 * np.pi * rows * out_t[None, :] / 32
    made["turn_low"] = planes([np.cos(turn), np.sin(turn)])

    grid = np.arange(512)
    t, group, part, source = grid >> 5, (grid >> 4) & 1, (grid >> 3) & 1, grid & 7
    number = np.where(group == 0, t, np.where(t == 0, 16, 32 - t))
    wave = 32 * source + number
    point = np.arange(LOW)[None, :]
    angle = 2 * np.pi * (wave[:, None] * point % LOW) / LOW
    weight = np.where(wave == 0, 1.0, np.where(wave < 128, 2.0, 0.0))
    weight = np.where((wave == 128) & (part == 0), 1.0, weight)
    value = np.where(part[:, None] == 0, np.cos(angle), -np.sin(angle))
    made["coarse_y"] = split_np(weight[:, None] * value, 0)
    away = np.arange(128)[:, None]
    own = np.arange(32)[None, :]
    parts = []
    for odd in range(2):
        place = 32 * away + 16 * odd - own
        kernel = 1.0 + 2.0 * sum(
            np.cos(2 * np.pi * (p * place % GRID) / GRID) for p in range(1, 128)
        )
        sign = 1.0 - 2.0 * odd
        edge = 2 * np.pi * own / 32 + 0 * away
        parts.append(
            np.concatenate([kernel + sign * np.cos(edge), sign * np.sin(edge)], axis=1)
        )
    scale = -(1 + coarse_ratio) * 0.5 * time_step / (64 * LOW)
    both = np.concatenate(parts, axis=0) * scale
    both = split_np(both, 1)
    high, low = both[:, :64], both[:, 64:]
    made["coarse_x"] = np.concatenate([high, high, low, 0 * low], axis=1)
    return made


def planes(parts):
    return np.concatenate(parts, axis=0).astype(np.float32)


def halves(values):
    high = values.astype(jnp.bfloat16)
    low = (values - high.astype(jnp.float32)).astype(jnp.bfloat16)
    return high, low


def dot(left_side, right_side):
    return jnp.dot(left_side, right_side, preferred_element_type=jnp.float32)


def thrice(table, axis):
    size = table.shape[axis] // 2
    high = lax.slice_in_dim(table, 0, size, axis=axis)
    low = lax.slice_in_dim(table, size, 2 * size, axis=axis)
    return jnp.concatenate([high, high, low], axis=axis)


def left_many(left_table, real, imag):
    count = len(real)
    stacked = jnp.concatenate(
        [jnp.concatenate(real, axis=1), jnp.concatenate(imag, axis=1)], axis=0
    )
    high, low = halves(stacked)
    out = dot(thrice(left_table, 1), jnp.concatenate([high, low, high], axis=0))
    cut = lambda row, place: out[row : row + 128, 128 * place : 128 * place + 128]
    return [cut(0, k) for k in range(count)], [cut(128, k) for k in range(count)]


def right_many(right_table, first, second):
    count = len(first)
    stacked = jnp.concatenate(
        [jnp.concatenate([a, b], axis=1) for a, b in zip(first, second)], axis=0
    )
    high, low = halves(stacked)
    out = dot(jnp.concatenate([high, low, high], axis=1), thrice(right_table, 0))
    cut = lambda row, col: out[128 * row : 128 * row + 128, col : col + 128]
    return [cut(k, 0) for k in range(count)], [cut(k, 128) for k in range(count)]


def lane_ids():
    return lax.broadcasted_iota(jnp.int32, (128, 128), 1)


def row_ids():
    return lax.broadcasted_iota(jnp.int32, (128, 128), 0)


def roll(block, shift):
    shift = shift % 128
    return block if shift == 0 else pltpu.roll(block, shift, 1)


def swap4(blocks):
    lane = lax.broadcasted_iota(jnp.int32, blocks[0].shape, 1)
    out = list(blocks)
    for bit, shift in ((0, 32), (1, 64)):
        low = ((lane >> (5 + bit)) & 1) == 0
        made = list(out)
        for index in range(4):
            if (index >> bit) & 1 == 0:
                a, b = out[index], out[index | (1 << bit)]
                made[index] = jnp.where(low, a, roll(b, shift))
                made[index | (1 << bit)] = jnp.where(low, roll(a, -shift), b)
        out = made
    return out


def turned(real, imag, cos, sin):
    return real * cos + imag * sin, imag * cos - real * sin


class Tables:
    def __init__(self, names, refs):
        self.refs = dict(zip(names, refs))

    def __getitem__(self, name):
        return self.refs[name][...]

    def turn(self, name, index):
        return self.refs[name][128 * index : 128 * index + 128, :]


def x_turned(tab, first, second):
    cos, sin = tab.turn("turn_x", 0), tab.turn("turn_x", 1)
    pairs = [turned(a, b, cos, sin) for a, b in zip(first, second)]
    return [p[0] for p in pairs], [p[1] for p in pairs]


def x_plain(tab, real, imag):
    real, imag = left_many(tab["left"], real, imag)
    return right_many(tab["right_x"], *x_turned(tab, real, imag))


def x_forward(tab, real, imag):
    return x_plain(tab, swap4(real), swap4(imag))


def x_inverse(tab, real, imag):
    first, second = right_many(tab["right_x"], imag, real)
    first, second = left_many(tab["left"], *x_turned(tab, first, second))
    return second, first


def y_forward(tab, groups):
    part0, part1 = right_many(
        tab["forward_y"], [g[0] for g in groups], [g[1] for g in groups]
    )
    start = lane_ids() < 8
    cos, sin = tab.turn("turn_y", 0), tab.turn("turn_y", 1)
    rest = jnp.where(start, 0.0, cos)
    real = [p * cos + q * sin for p, q in zip(part0, part1)]
    imag = [q * rest - p * sin for p, q in zip(part0, part1)]
    direct = left_many(tab["left"], real, imag)
    cos, sin = tab.turn("turn_y", 2), tab.turn("turn_y", 3)
    a, b = jnp.where(start, 0.0, cos), jnp.where(start, cos, -sin)
    d, e = jnp.where(start, 0.0, -sin), jnp.where(start, -sin, -cos)
    real = [p * a + q * b for p, q in zip(part0, part1)]
    imag = [p * d + q * e for p, q in zip(part0, part1)]
    mirror = left_many(tab["left"], real, imag)
    return direct, mirror


def y_inverse(tab, real, imag, edge, place):
    imag, real = left_many(tab["left"], imag, real)
    start = lane_ids() < 8
    cos, sin = 2.0 * tab.turn("turn_y", 0), 2.0 * tab.turn("turn_y", 1)
    parts = [
        [p * cos - q * sin for p, q in zip(real, imag)],
        [p * sin + q * cos for p, q in zip(real, imag)],
    ]
    for part, values in zip(parts, edge):
        for xh in range(4):
            part[xh] = jnp.where(start, roll(values, -(32 * xh + 8 * place)), part[xh])
    return right_many(tab["inverse_y"], *parts)


def edge_rows(tab, sets):
    lane = lane_ids()
    packed = [0.0, 0.0]
    for place, both in enumerate(sets):
        for part, blocks in enumerate(both):
            for xh in range(4):
                mine = (lane >> 3) == 4 * xh + place
                moved = roll(blocks[xh], 32 * xh + 8 * place)
                packed[part] = jnp.where(mine, moved, packed[part])
    first, second = left_many(tab["left_edge"], [packed[0]], [packed[1]])
    return first[0], second[0]


def load(ref, index, count):
    return ref[pl.ds(index, 128, stride=count), :]


def store(ref, index, count, block):
    ref[pl.ds(index, 128, stride=count), :] = block


def load_set(ref, base, count):
    real = [load(ref, base + k, count) for k in range(4)]
    imag = [load(ref, base + 4 + k, count) for k in range(4)]
    return real, imag


def store_set(ref, base, count, real, imag):
    for k in range(4):
        store(ref, base + k, count, real[k])
        store(ref, base + 4 + k, count, imag[k])


def block(ref, index):
    return ref[128 * index : 128 * index + 128, :]


def put(ref, index, value):
    ref[128 * index : 128 * index + 128, :] = value


def rank_here():
    return lax.axis_index("gx") * lax.axis_size("gy") + lax.axis_index("gy")


class Rows:
    def __init__(self, rank, group, quarter):
        lane = lax.broadcasted_iota(jnp.int32, (1, 128), 1)
        slot = 4 * quarter + ((lane >> 3) & 3)
        if group == 1:
            slot = jnp.where(slot == 0, 16, 32 - slot)
        if group == 2:
            slot = jnp.where((slot == 0) & (rank >= 64), 16, slot)
        row = 32 * rank + slot
        my = jnp.where(row < GRID // 2, row, row - GRID)
        self.my = my
        self.square = (my * my).astype(jnp.float32)
        self.slope = jnp.where(row == GRID // 2, 0, my).astype(jnp.float32) * unit

    def keep(self, cutoff):
        return jnp.where(jnp.abs(self.my) <= cutoff, 1.0, 0.0)

    def low(self):
        half = LOW // 2
        return jnp.where((self.my >= -half) & (self.my < half), 1.0, 0.0)


def keep_columns(tab, cutoff):
    return jnp.where(tab.turn("wave_x", 1) <= (cutoff * cutoff).astype(jnp.float32), 1.0, 0.0)


def send_fields(tab, rank, state, hidden, out_ref, count, names):
    rows = [Rows(rank, 2, q) for q in range(4)]
    across, squares = tab.turn("wave_x", 0), tab.turn("wave_x", 1)
    sources = {}
    for index in range(4):
        real, imag = state(0, index)
        if index == 0:
            upper = first_slot() & (rank >= 64)
            real, imag = [
                jnp.where(upper, other, own) for own, other in zip((real, imag), state(1, 0))
            ]
        both = squares + rows[index].square
        scale = jnp.where(both == 0.0, 0.0, (1.0 / (unit * unit)) / jnp.maximum(both, 1.0))
        sources["w", index] = real, imag
        sources["psi", index] = real * scale, imag * scale
    scale = (1.0 / (unit * unit)) / (squares + float((GRID // 2) ** 2))
    for place, name in enumerate(names):
        reals, imags = [], []
        for index in range(4):
            real, imag = sources["psi" if name in ("u", "v") else "w", index]
            factor = rows[index].slope if name in ("u", "wy") else across
            if name == "v":
                reals.append(imag * factor)
                imags.append(-real * factor)
            else:
                reals.append(-imag * factor)
                imags.append(real * factor)
        if name in ("v", "wx"):
            factor = across * scale if name == "v" else -across
            reals[0] = reals[0] + hidden[0] * factor
            imags[0] = imags[0] + hidden[1] * factor
        real, imag = x_inverse(tab, reals, imags)
        store_set(out_ref, 8 * place, count, swap4(real), swap4(imag))


def first_slot():
    return ((lane_ids() >> 3) & 3) == 0


def split_rows(tab, rank, real, imag):
    flip = tab["flip"]
    sub = row_ids()
    both = jnp.concatenate([real, imag], axis=0)
    high, low = halves(both)
    pair = jnp.concatenate([high, low], axis=1)
    twice = lambda table, axis: jnp.concatenate([table, table], axis=axis)
    most = dot(pair, twice(flip[:128], 0))
    top = dot(pair, twice(flip[128:256], 0))
    wide = jnp.concatenate([most[:128], most[128:]], axis=1)
    high, low = halves(wide)
    wide = dot(twice(flip[256:], 1), jnp.concatenate([high, low], axis=0))
    real_back = jnp.where(sub == 0, top[:128], wide[:, :128])
    imag_back = jnp.where(sub == 0, top[128:], wide[:, 128:])
    mine = first_slot() & (rank == 0)
    own = [
        jnp.where(mine, 0.5 * (real + real_back), real),
        jnp.where(mine, 0.5 * (imag - imag_back), imag),
    ]
    hidden = [
        jnp.where(mine, 0.5 * (imag + imag_back), 0.0),
        jnp.where(mine, 0.5 * (real_back - real), 0.0),
    ]
    return own, hidden


FIRST = ("left", "forward_y", "turn_y", "low_rows", "turn_low")
WAVES = ("left", "right_x", "turn_x", "wave_x")
START = WAVES + ("flip",)
MIDDLE = WAVES + ("half",)
FINAL = WAVES + ("coarse_rows", "coarse_turn")
ROWS = ("left", "left_edge", "forward_y", "inverse_y", "turn_y")
PRODUCT = ROWS + ("drive_spots",)
LAST = ROWS + ("coarse_y", "coarse_x")


def grid_groups(ref):
    groups = []
    for xh in range(4):
        pair = []
        for jh in range(2):
            pieces = [
                ref[8 * xh : 8 * xh + 8, 128 * j : 128 * j + 128]
                for j in range(16 * jh, 16 * jh + 16)
            ]
            pair.append(jnp.concatenate(pieces, axis=0).T)
        groups.append(pair)
    return groups


def first_kernel(*rest):
    total = 2 + len(FIRST)
    out_ref, *held, ready = rest[total + 1 :]
    copies = {}
    for name in ("rows", "forward_y", "turn_y", "left", "force", "low_rows", "turn_low"):
        k = ("rows", "force").index(name) if name in ("rows", "force") else 2 + FIRST.index(name)
        copies[name] = pltpu.make_async_copy(rest[k], held[k], ready.at[k])
        copies[name].start()
    vorticity_ref, forcing_ref = held[:2]
    tab = Tables(FIRST, held[2:])
    for name in ("rows", "forward_y", "turn_y", "left"):
        copies[name].wait()
    direct, mirror = y_forward(tab, grid_groups(vorticity_ref))
    lane, row = lane_ids(), row_ids()
    spot = (lane < 8) & (row == 0)
    real, imag = direct
    imag = [
        jnp.where(spot, jnp.broadcast_to(p[64:65, :], (128, 128)), q)
        for p, q in zip(real, imag)
    ]
    store_set(out_ref, 0, 17, real, imag)
    store_set(out_ref, 8, 17, *mirror)
    for name in ("force", "low_rows", "turn_low"):
        copies[name].wait()
    groups = grid_groups(forcing_ref)
    values = jnp.concatenate([g[k] for g in groups for k in range(2)], axis=1)
    high, low = halves(values)
    out = dot(thrice(tab["low_rows"], 1), jnp.concatenate([high, low, high], axis=0))
    lane, row = lane_ids(), row_ids()
    sign = jnp.where((row & 1) == 0, 1.0, -1.0)
    cos, sin = tab.turn("turn_low", 0), tab.turn("turn_low", 1)
    packed = jnp.zeros((128, 128), jnp.float32)
    for xh in range(4):
        at = 256 * xh
        real = out[:128, at : at + 128] + sign * out[:128, at + 128 : at + 256]
        imag = out[128:, at : at + 128] + sign * out[128:, at + 128 : at + 256]
        for part, value in enumerate(turned(real, imag, cos, sin)):
            for shift in (64, 32, 16, 8):
                value = value + roll(value, shift)
            mine = ((lane >> 5) == xh) & (((lane >> 3) & 3) == part)
            packed = jnp.where(mine, value, packed)
    store(out_ref, 16, 17, packed)


def start_kernel(in_ref, *rest):
    tab = Tables(START, rest)
    state_ref, out_ref = rest[len(START) :]
    rank = rank_here()
    for group in range(2):
        real, imag = x_forward(tab, *load_set(in_ref, 8 * group, 17))
        if group == 0:
            (real[0], imag[0]), hidden = split_rows(tab, rank, real[0], imag[0])
            put(state_ref, 16, hidden[0])
            put(state_ref, 17, hidden[1])
        for q in range(4):
            put(state_ref, 8 * group + 2 * q, real[q])
            put(state_ref, 8 * group + 2 * q + 1, imag[q])
    row = load(in_ref, 16, 17)
    lane = lane_ids()
    part = (lane >> 3) & 3
    real = jnp.where(part == 0, row, jnp.where(part == 1, roll(row, 8), 0.0))
    imag = jnp.where(part == 0, roll(row, -8), jnp.where(part == 1, -row, 0.0))
    real, imag = x_plain(tab, [real], [imag])

    packed = jnp.zeros((128, 128), jnp.float32)
    for which, source in enumerate((real[0], imag[0])):
        for spot, origin in enumerate((0, 103, 8, 111)):
            at = 4 * which + spot
            packed = jnp.where(lane == at, roll(source, at - origin), packed)
    store(out_ref, 24, 25, packed)

    state = lambda group, q: (
        block(state_ref, 8 * group + 2 * q),
        block(state_ref, 8 * group + 2 * q + 1),
    )
    hidden = block(state_ref, 16), block(state_ref, 17)
    send_fields(tab, rank, state, hidden, out_ref, 25, ("u", "v", "wx"))


def product_one(tab, in_ref, count, edge, place):
    real, imag = load_set(in_ref, 8 * place, count)
    return y_inverse(tab, real, imag, edge, place)


def drive_rows(tab, values):
    columns = values.T
    pick = lambda index: jnp.broadcast_to(columns[index : index + 1, :], (8, 128))
    plus = swap4([pick(4 * part + k) for part in range(2) for k in range(2)])
    minus = swap4([pick(4 * part + 2 + k) for part in range(2) for k in range(2)])
    sub = lax.broadcasted_iota(jnp.int32, (8, 128), 0)
    start = (lax.broadcasted_iota(jnp.int32, (8, 128), 1) & 31) == 0
    top = jnp.zeros((8, 128), jnp.float32)
    bottom = jnp.zeros((8, 128), jnp.float32)
    for k in range(4):
        top = jnp.where(sub == k, plus[k], top)
        after = minus[k + 1] if k < 3 else 0.0
        bottom = jnp.where(sub == 7 - k, jnp.where(start, after, minus[k]), bottom)
    spots = tab["drive_spots"]
    made = []
    for values, table in ((top, spots[:128]), (bottom, spots[128:])):
        high, low = halves(values)
        made.append(dot(high, table) + dot(low, table))
    return jnp.concatenate([made[0], jnp.zeros((112, 128), jnp.float32), made[1]], axis=0)


def product_first_kernel(in_ref, local_ref, *rest):
    tab = Tables(PRODUCT, rest)
    out_ref = rest[len(PRODUCT)]
    store(out_ref, 16, 17, drive_rows(tab, load(in_ref, 24, 25)))
    lane = lane_ids()
    upper = (lane < 8) & (row_ids() >= 64)
    row = 32 * row_ids() + jnp.where(upper, 16, lane >> 3)
    slope = jnp.where(row < GRID // 2, row, row - GRID)
    slope = jnp.where(row == GRID // 2, 0, slope).astype(jnp.float32) * unit
    real, imag = load_set(local_ref, 0, 17)
    other_real, other_imag = load_set(local_ref, 8, 17)
    own = (
        [-slope * jnp.where(upper, b, a) for a, b in zip(imag, other_imag)],
        [slope * jnp.where(upper, b, a) for a, b in zip(real, other_real)],
    )
    last = edge_rows(tab, [load_set(in_ref, 8 * k, 25) for k in range(3)] + [own])
    u0, u1 = product_one(tab, in_ref, 25, last, 0)
    x0, x1 = product_one(tab, in_ref, 25, last, 2)
    sum0 = [a * b for a, b in zip(u0, x0)]
    sum1 = [a * b for a, b in zip(u1, x1)]
    y0, y1 = y_inverse(tab, *own, last, 3)
    v0, v1 = product_one(tab, in_ref, 25, last, 1)
    sum0 = [s + a * b for s, a, b in zip(sum0, v0, y0)]
    sum1 = [s + a * b for s, a, b in zip(sum1, v1, y1)]
    direct, mirror = y_forward(tab, list(zip(sum0, sum1)))
    store_set(out_ref, 0, 17, *direct)
    store_set(out_ref, 8, 17, *mirror)


def product_kernel(in_ref, *rest):
    tab = Tables(LAST, rest)
    out_ref, mixed_ref = rest[len(LAST) :]
    got = load(in_ref, 32, 33)
    mixed_ref[0:4, :] = got[0:4, :]
    mixed_ref[4:8, :] = got[124:128, :]
    last = edge_rows(tab, [load_set(in_ref, 8 * k, 33) for k in range(4)])
    sum0, sum1 = None, None
    for one, two in ((0, 2), (1, 3)):
        a0, a1 = product_one(tab, in_ref, 33, last, one)
        b0, b1 = product_one(tab, in_ref, 33, last, two)
        made0 = [a * b for a, b in zip(a0, b0)]
        made1 = [a * b for a, b in zip(a1, b1)]
        sum0 = made0 if sum0 is None else [s + m for s, m in zip(sum0, made0)]
        sum1 = made1 if sum1 is None else [s + m for s, m in zip(sum1, made1)]
    direct, mirror = y_forward(tab, list(zip(sum0, sum1)))
    store_set(out_ref, 0, 20, *direct)
    store_set(out_ref, 8, 20, *mirror)
    pieces = []
    for xh in range(4):
        for part in (direct[0], direct[1], mirror[0], mirror[1]):
            pieces.append(part[xh][0:8, :])
    across = jnp.concatenate(pieces, axis=0).T
    made = [
        swap4([across[8 * t : 8 * t + 8, :] for t in range(4 * tq, 4 * tq + 4)])
        for tq in range(4)
    ]
    values = jnp.concatenate(
        [jnp.concatenate([made[tq][xh] for tq in range(4)], axis=1) for xh in range(4)],
        axis=0,
    )
    high, low = halves(values)
    points = dot(
        jnp.concatenate([high, low, high], axis=1), thrice(tab["coarse_y"], 0)
    )
    flip = lax.broadcasted_iota(jnp.int32, (32, LOW), 1) & 1
    edge = jnp.where(flip == 0, 1.0, -1.0) * values[:, 12:13]
    high, low = halves(jnp.concatenate([points, edge], axis=0))
    share = dot(
        tab["coarse_x"], jnp.concatenate([high, low, high, jnp.zeros_like(low)], axis=0)
    )
    for odd in range(2):
        for side in range(2):
            piece = share[128 * odd : 128 * odd + 128, 128 * side : 128 * side + 128]
            piece = pltpu.roll(piece, rank_here(), 0)
            store(out_ref, 16 + 2 * odd + side, 20, piece)


def shelled(rank, values, radii):
    lane = lane_ids()
    side, spot = (lane >> 5) & 1, lane & 7
    slot = 4 * (spot & 3) + ((lane >> 3) & 3)
    slot = jnp.where(spot < 4, slot, jnp.where(slot == 0, 16, 32 - slot))
    my = 32 * rank + slot
    my = jnp.where(my < GRID // 2, my, my - GRID)
    mx = row_ids() - 128 * side
    squares = mx * mx + my * my
    mask = None
    for radius in radii:
        inside = (radius * radius <= squares) & (squares < (radius + 1) * (radius + 1))
        mask = inside if mask is None else mask | inside
    return jnp.where(mask, values, 0.0)


def fetch(ready, pairs):
    copies = [
        pltpu.make_async_copy(source, target, ready.at[k])
        for k, (source, target) in enumerate(pairs)
    ]
    for copy in copies:
        copy.start()
    return copies


def middle_kernel(cutoff_from, shells_from, in_ref, state_ref, *rest):
    tab = Tables(MIDDLE, rest)
    ahead_ref, out_ref, next_ref, cutoff_ref, shells_ref, ready = rest[len(MIDDLE) :]
    copies = fetch(ready, ((cutoff_from, cutoff_ref), (shells_from, shells_ref)))
    rank = rank_here()
    lane = lane_ids()
    spectra = [x_forward(tab, *load_set(in_ref, 8 * group, 17)) for group in range(2)]
    for copy in copies:
        copy.wait()
    cutoff = cutoff_ref[0]
    forcing = shelled(rank, load(in_ref, 16, 17), [shells_ref[k] for k in range(SHELLS)])
    first_spots = (lane < 32) & ((lane & 7) == 0)
    last_spots = (lane >= 96) & ((lane & 7) == 7)
    keep_x = keep_columns(tab, cutoff)
    squares, low_x = tab.turn("wave_x", 1), tab.turn("wave_x", 2)
    low0 = [0.0, 0.0]
    low1 = [0.0, 0.0]
    for group in range(2):
        real, imag = spectra[group]
        for q in range(4):
            rows = Rows(rank, group, q)
            keep = keep_x * rows.keep(cutoff)
            low = low_x * rows.low()
            damp = (viscosity * unit * unit) * (squares + rows.square)
            spot = 4 * group + q
            mine = (lane < 32) & ((lane & 7) == spot)
            for part, term in enumerate((real[q], imag[q])):
                place = 8 * group + 2 * q + part
                now = block(state_ref, place)
                drive = jnp.where(first_spots, roll(forcing, -64 * part - spot), 0.0)
                drive = jnp.where(
                    last_spots, roll(forcing, 71 - 64 * part - spot), drive
                )
                slope = drive - keep * term - damp * now
                after = now + time_step * slope
                if place < 10:
                    put(next_ref, place, after)
                rest_slope = slope + drive - damp * after
                change = 0.5 * time_step * rest_slope
                lifted = now + change + (coarse_ratio * low) * change
                put(ahead_ref, place, lifted)
                lifted = low * lifted
                low0[part] = jnp.where(mine, roll(lifted, spot), low0[part])
                low1[part] = jnp.where(mine, roll(lifted, 25 + spot), low1[part])
    even = [a + b for a, b in zip(low0, low1)]
    odd = [a - b for a, b in zip(low0, low1)]
    cos, sin = tab.turn("half", 0), tab.turn("half", 1)
    odd = [odd[0] * cos - odd[1] * sin, odd[0] * sin + odd[1] * cos]
    both = [jnp.where(lane < 32, e, roll(o, 32)) for e, o in zip(even, odd)]
    both = [jnp.where(lane < 64, b, 0.0) for b in both]
    second, first = left_many(tab["left"], [both[1]], [both[0]])
    store(out_ref, 32, 33, jnp.where(lane < 64, first[0], roll(second[0], 64)))
    state = lambda group, q: (
        block(next_ref, 8 * group + 2 * q),
        block(next_ref, 8 * group + 2 * q + 1),
    )
    damp = (viscosity * unit * unit) * (squares + float((GRID // 2) ** 2))
    fade = 1.0 - time_step * damp
    hidden = block(state_ref, 16) * fade, block(state_ref, 17) * fade
    send_fields(tab, rank, state, hidden, out_ref, 33, ("u", "v", "wx", "wy"))


def final_kernel(cutoff_from, in_ref, ahead_ref, mixed_ref, *rest):
    tab = Tables(FINAL, rest)
    out_ref, points_ref, held_ref, cutoff_ref, ready, done_ref = rest[len(FINAL) :]
    (copy,) = fetch(ready, ((cutoff_from, cutoff_ref),))
    rank = rank_here()
    spectra = [x_forward(tab, *load_set(in_ref, 8 * group, 20)) for group in range(2)]
    copy.wait()
    cutoff = cutoff_ref[0]
    keep_x = keep_columns(tab, cutoff) * (0.5 * time_step)
    low_x = tab.turn("wave_x", 2) * coarse_ratio
    copies = []
    for group in range(2):
        real, imag = spectra[group]
        for q in range(4):
            rows = Rows(rank, group, q)
            factor = keep_x * rows.keep(cutoff)
            factor = factor + factor * (low_x * rows.low())
            for part, term in enumerate((real[q], imag[q])):
                lifted = block(ahead_ref, 8 * group + 2 * q + part) - factor * term
                flipped = lifted.T
                for kh in range(4):
                    for slot in range(4):
                        at = 32 * kh + 8 * slot
                        piece = flipped[at : at + 8, :]
                        number = 4 * q + slot
                        if group == 1:
                            number = 16 if number == 0 else 32 - number
                        for kl in range(8):
                            col = 128 * (8 * kh + kl)
                            held_ref[part, number, col : col + 128] = piece[kl]
        for part in range(2):
            spot = (part, slice(16 * group, 16 * group + 16))
            copies.append(
                pltpu.make_async_copy(
                    held_ref.at[spot], out_ref.at[spot], done_ref.at[2 * group + part]
                )
            )
            copies[-1].start()
    mixed = mixed_ref[...]
    high, low = halves(jnp.concatenate([mixed, roll(mixed, -32)], axis=0))
    out = dot(
        jnp.concatenate([high, low, high], axis=1), thrice(tab["coarse_rows"], 0)
    )
    turn = tab["coarse_turn"]
    for odd in range(2):
        rows = out[8 * odd : 8 * odd + 8]
        rows = rows[:, :LOW] * turn[:8] + rows[:, LOW:] * turn[8:]
        line = jnp.sum(rows, axis=0, keepdims=True)
        for side in range(2):
            total = jnp.sum(load(in_ref, 16 + 2 * odd + side, 20), axis=0, keepdims=True)
            at = slice(128 * side, 128 * side + 128)
            points_ref[odd : odd + 1, at] = line[:, at] + total
    for copy in copies:
        copy.wait()


VMEM = pl.BlockSpec(memory_space=pltpu.VMEM)


HBM = pl.BlockSpec(memory_space=pltpu.HBM)


def call(kernel, name, outs, args, far=(), out_specs=None, scratch=()):
    far = tuple(
        a if a.ndim == 1 else pltpu.with_memory_space_constraint(a, pltpu.HBM) for a in far
    )
    return pl.pallas_call(
        kernel,
        name=name,
        out_shape=[jax.ShapeDtypeStruct(shape, jnp.float32) for shape in outs],
        in_specs=[HBM] * len(far) + [VMEM] * len(args),
        out_specs=out_specs or [VMEM] * len(outs),
        scratch_shapes=list(scratch),
        compiler_params=pltpu.CompilerParams(vmem_limit_bytes=VMEM_LIMIT * 1024 * 1024),
    )(*far, *args)


def near(array):
    return pltpu.with_memory_space_constraint(array, pltpu.VMEM)


def exchange(buffer, count):
    cut = buffer.reshape(128, 1, count * 128)
    cut = lax.all_to_all(cut, AXES, split_axis=0, concat_axis=0, tiled=True)
    return cut.reshape(128 * count, 128)


def body(vorticity_grid, forcing_grid, cutoff, forcing_shells):
    made = {name: jnp.asarray(table) for name, table in tables().items()}
    tabs = lambda names: tuple(made[name] for name in names)
    spectrum = (16 * 128, 128)
    args = (vorticity_grid, forcing_grid) + tabs(FIRST)
    (sent,) = call(
        first_kernel,
        "first",
        [(128 * 17, 128)],
        (),
        args + (cutoff,),
        scratch=[pltpu.VMEM(a.shape, a.dtype) for a in args]
        + [pltpu.SemaphoreType.DMA((len(args),))],
    )
    got = exchange(sent, 17)
    state, fields = call(
        start_kernel, "start", [(18 * 128, 128), (128 * 25, 128)], (got,) + tabs(START)
    )
    got = exchange(fields, 25)
    (term,) = call(
        product_first_kernel, "product_first", [(128 * 17, 128)], (got, near(sent)) + tabs(PRODUCT)
    )
    got = exchange(term, 17)
    ahead, fields = call(
        middle_kernel,
        "middle",
        [spectrum, (128 * 33, 128)],
        (got, near(state)) + tabs(MIDDLE),
        (cutoff, forcing_shells),
        scratch=[
            pltpu.VMEM((10 * 128, 128), jnp.float32),
            pltpu.SMEM((1,), jnp.int32),
            pltpu.SMEM((SHELLS,), jnp.int32),
            pltpu.SemaphoreType.DMA((2,)),
        ],
    )
    got = exchange(fields, 33)
    term, mixed = call(
        product_kernel, "product", [(128 * 20, 128), (8, 128)], (got,) + tabs(LAST)
    )
    got = exchange(term, 20)
    lifted, coarse = call(
        final_kernel,
        "final",
        [(2, 32, GRID), (2, LOW)],
        (got, near(ahead), mixed) + tabs(FINAL),
        (cutoff,),
        out_specs=[HBM, VMEM],
        scratch=[
            pltpu.VMEM((2, 32, GRID), jnp.float32),
            pltpu.SMEM((1,), jnp.int32),
            pltpu.SemaphoreType.DMA((1,)),
            pltpu.SemaphoreType.DMA((4,)),
        ],
    )
    return lifted, coarse


def solution(mesh):
    placed = (P(AXES, None), P(AXES, None), P(), P())
    return jax.shard_map(
        body,
        mesh=mesh,
        in_specs=placed,
        out_specs=(P(None, AXES, None), P(AXES, None)),
        check_vma=False,
    )
```

```python
import functools
import math

import jax
import jax.numpy as jnp
import numpy as np
from jax import lax
from jax.experimental import pallas as pl
from jax.experimental.pallas import tpu as pltpu
from jax.sharding import PartitionSpec as P

GRID = 4096
LANES = 128
LOW = 256
SHELLS = 4
VMEM_LIMIT = 24
AXES = ("gx", "gy")

time_step = 0.05
viscosity = 0.05
coarse_ratio = 4.0
unit = 2.0 * math.pi / GRID


def split_np(table, axis):
    high = table.astype(np.float32).astype(jnp.bfloat16)
    low = (table - high.astype(np.float64)).astype(np.float32).astype(jnp.bfloat16)
    return np.concatenate([high, low], axis=axis)


@functools.lru_cache(None)
def tables():
    made = {}
    index = np.arange(128)
    rows = index[:, None]
    angle = 2 * np.pi * np.outer(index, index) / 128
    cos, sin = np.cos(angle) / 8, np.sin(angle) / 8
    made["left"] = split_np(np.block([[cos, sin], [-sin, cos]]), 1)

    near = (index >= 1) & (index < 64)
    far = index >= 64
    angle = 2 * np.pi * np.outer(index, index) / 128
    later = 2 * np.pi * np.outer(index, index + 0.5) / 128
    real = np.where(near, 2 * np.cos(angle), np.where(index == 0, 1.0, 0.0))
    imag = np.where(near, -2 * np.sin(angle), np.where(index == 0, (-1.0) ** rows, 0.0))
    edge = [[real, imag], [far * 2 * np.cos(later), far * -2 * np.sin(later)]]
    made["left_edge"] = split_np(np.block(edge) / 8, 1)

    lane = np.arange(128)
    inner = 8 * (lane >> 5) + (lane & 7)
    slot = (lane >> 3) & 3
    same = slot[:, None] == slot[None, :]
    angle = 2 * np.pi * np.outer(inner, inner) / 32
    cos, sin = same * np.cos(angle) / 8, same * np.sin(angle) / 8
    made["right_x"] = split_np(np.block([[cos, -sin], [sin, cos]]), 0)

    wide = np.arange(256)
    col_j, col_x = wide >> 3, wide & 7
    out_t, out_x = lane >> 3, lane & 7
    same = col_x[:, None] == out_x[None, :]
    angle = 2 * np.pi * np.outer(col_j, out_t) / 32
    part0 = np.cos(angle)
    part1 = -np.sin(angle)
    part1[:, out_t == 0] = np.where(col_j % 2 == 0, 1.0, -1.0)[:, None]
    right_y = np.concatenate([same * part0, same * part1], axis=1) / 8
    made["forward_y"] = split_np(right_y, 0)
    made["inverse_y"] = split_np(right_y.T, 0)

    turn = 2 * np.pi * rows * inner[None, :] / GRID
    made["turn_x"] = planes([np.cos(turn), np.sin(turn)])
    turn_d = 2 * np.pi * rows * out_t[None, :] / GRID
    back = np.where(out_t == 0, 16, 32 - out_t)
    turn_m = 2 * np.pi * rows * back[None, :] / GRID
    made["turn_y"] = planes([np.cos(turn_d), np.sin(turn_d), np.cos(turn_m), np.sin(turn_m)])
    half = 2 * np.pi * rows / 256 + np.zeros((128, 128))
    made["half"] = planes([np.cos(half), np.sin(half)])

    column = rows + 128 * inner[None, :]
    mx = np.where(column < GRID // 2, column, column - GRID)
    made["wave_x"] = planes(
        [
            np.where(column == GRID // 2, 0, mx) * unit,
            mx * mx,
            np.where((mx >= -LOW // 2) & (mx < LOW // 2), 1.0, 0.0),
        ]
    )

    spot = np.arange(32)
    inside, group, quarter = spot >> 3, (spot >> 2) & 1, spot & 3
    number = 4 * quarter + inside
    number = np.where(group == 0, number, np.where(number == 0, 16, 32 - number))
    made["drive_spots"] = np.concatenate(
        [
            np.kron(np.eye(4), index[:32, None] == want[None, :])
            for want in (number, (32 - number) % 32)
        ],
        axis=0,
    ).astype(jnp.bfloat16)

    point = np.arange(LOW)[None, :]
    angle = 2 * np.pi * (np.tile(number, 4)[:, None] * point % LOW) / LOW
    plain = ((lane >> 5) & 1 == 0)[:, None] * (8 / LOW)
    imag = (lane >= 64)[:, None]
    made["coarse_rows"] = split_np(
        np.concatenate(
            [
                plain * np.where(imag, -np.sin(angle), np.cos(angle)),
                plain * np.where(imag, np.cos(angle), np.sin(angle)),
            ],
            axis=1,
        ),
        0,
    )
    source = np.array([0, 1, 2, 3, 124, 125, 126, 127])[:, None]
    angle = 2 * np.pi * (source * point % 8) / 8
    made["coarse_turn"] = planes([np.cos(angle), -np.sin(angle)])

    flips = [
        (slot[:, None] == slot[None, :]) & (inner[:, None] == want[None, :])
        for want in (31 - inner, (32 - inner) % 32)
    ]
    flips.append(rows == (128 - index[None, :]) % 128)
    made["flip"] = np.concatenate(flips, axis=0).astype(np.float32).astype(jnp.bfloat16)

    angle = 2 * np.pi * np.outer(index, index) / GRID
    low = np.concatenate([np.cos(angle), -np.sin(angle)], axis=0) / 64
    made["low_rows"] = split_np(low, 1)
    turn = 2 * np.pi * rows * out_t[None, :] / 32
    made["turn_low"] = planes([np.cos(turn), np.sin(turn)])

    grid = np.arange(512)
    t, group, part, source = grid >> 5, (grid >> 4) & 1, (grid >> 3) & 1, grid & 7
    number = np.where(group == 0, t, np.where(t == 0, 16, 32 - t))
    wave = 32 * source + number
    point = np.arange(LOW)[None, :]
    angle = 2 * np.pi * (wave[:, None] * point % LOW) / LOW
    weight = np.where(wave == 0, 1.0, np.where(wave < 128, 2.0, 0.0))
    weight = np.where((wave == 128) & (part == 0), 1.0, weight)
    value = np.where(part[:, None] == 0, np.cos(angle), -np.sin(angle))
    made["coarse_y"] = split_np(weight[:, None] * value, 0)
    away = np.arange(128)[:, None]
    own = np.arange(32)[None, :]
    parts = []
    for odd in range(2):
        place = 32 * away + 16 * odd - own
        kernel = 1.0 + 2.0 * sum(
            np.cos(2 * np.pi * (p * place % GRID) / GRID) for p in range(1, 128)
        )
        sign = 1.0 - 2.0 * odd
        edge = 2 * np.pi * own / 32 + 0 * away
        parts.append(
            np.concatenate([kernel + sign * np.cos(edge), sign * np.sin(edge)], axis=1)
        )
    scale = -(1 + coarse_ratio) * 0.5 * time_step / (64 * LOW)
    both = np.concatenate(parts, axis=0) * scale
    both = split_np(both, 1)
    high, low = both[:, :64], both[:, 64:]
    made["coarse_x"] = np.concatenate([high, high, low, 0 * low], axis=1)
    return made


def planes(parts):
    return np.concatenate(parts, axis=0).astype(np.float32)


def halves(values):
    high = values.astype(jnp.bfloat16)
    low = (values - high.astype(jnp.float32)).astype(jnp.bfloat16)
    return high, low


def dot(left_side, right_side):
    return jnp.dot(left_side, right_side, preferred_element_type=jnp.float32)


def thrice(table, axis):
    size = table.shape[axis] // 2
    high = lax.slice_in_dim(table, 0, size, axis=axis)
    low = lax.slice_in_dim(table, size, 2 * size, axis=axis)
    return jnp.concatenate([high, high, low], axis=axis)


def left_many(left_table, real, imag):
    count = len(real)
    stacked = jnp.concatenate(
        [jnp.concatenate(real, axis=1), jnp.concatenate(imag, axis=1)], axis=0
    )
    high, low = halves(stacked)
    out = dot(thrice(left_table, 1), jnp.concatenate([high, low, high], axis=0))
    cut = lambda row, place: out[row : row + 128, 128 * place : 128 * place + 128]
    return [cut(0, k) for k in range(count)], [cut(128, k) for k in range(count)]


def right_many(right_table, first, second):
    count = len(first)
    stacked = jnp.concatenate(
        [jnp.concatenate([a, b], axis=1) for a, b in zip(first, second)], axis=0
    )
    high, low = halves(stacked)
    out = dot(jnp.concatenate([high, low, high], axis=1), thrice(right_table, 0))
    cut = lambda row, col: out[128 * row : 128 * row + 128, col : col + 128]
    return [cut(k, 0) for k in range(count)], [cut(k, 128) for k in range(count)]


def lane_ids():
    return lax.broadcasted_iota(jnp.int32, (128, 128), 1)


def row_ids():
    return lax.broadcasted_iota(jnp.int32, (128, 128), 0)


def roll(block, shift):
    shift = shift % 128
    return block if shift == 0 else pltpu.roll(block, shift, 1)


def swap4(blocks):
    lane = lax.broadcasted_iota(jnp.int32, blocks[0].shape, 1)
    out = list(blocks)
    for bit, shift in ((0, 32), (1, 64)):
        low = ((lane >> (5 + bit)) & 1) == 0
        made = list(out)
        for index in range(4):
            if (index >> bit) & 1 == 0:
                a, b = out[index], out[index | (1 << bit)]
                made[index] = jnp.where(low, a, roll(b, shift))
                made[index | (1 << bit)] = jnp.where(low, roll(a, -shift), b)
        out = made
    return out


def turned(real, imag, cos, sin):
    return real * cos + imag * sin, imag * cos - real * sin


class Tables:
    def __init__(self, names, refs):
        self.refs = dict(zip(names, refs))

    def __getitem__(self, name):
        return self.refs[name][...]

    def turn(self, name, index):
        return self.refs[name][128 * index : 128 * index + 128, :]


def x_turned(tab, first, second):
    cos, sin = tab.turn("turn_x", 0), tab.turn("turn_x", 1)
    pairs = [turned(a, b, cos, sin) for a, b in zip(first, second)]
    return [p[0] for p in pairs], [p[1] for p in pairs]


def x_plain(tab, real, imag):
    real, imag = left_many(tab["left"], real, imag)
    return right_many(tab["right_x"], *x_turned(tab, real, imag))


def x_forward(tab, real, imag):
    return x_plain(tab, swap4(real), swap4(imag))


def x_inverse(tab, real, imag):
    first, second = right_many(tab["right_x"], imag, real)
    first, second = left_many(tab["left"], *x_turned(tab, first, second))
    return second, first


def y_forward(tab, groups):
    part0, part1 = right_many(
        tab["forward_y"], [g[0] for g in groups], [g[1] for g in groups]
    )
    start = lane_ids() < 8
    cos, sin = tab.turn("turn_y", 0), tab.turn("turn_y", 1)
    rest = jnp.where(start, 0.0, cos)
    real = [p * cos + q * sin for p, q in zip(part0, part1)]
    imag = [q * rest - p * sin for p, q in zip(part0, part1)]
    direct = left_many(tab["left"], real, imag)
    cos, sin = tab.turn("turn_y", 2), tab.turn("turn_y", 3)
    a, b = jnp.where(start, 0.0, cos), jnp.where(start, cos, -sin)
    d, e = jnp.where(start, 0.0, -sin), jnp.where(start, -sin, -cos)
    real = [p * a + q * b for p, q in zip(part0, part1)]
    imag = [p * d + q * e for p, q in zip(part0, part1)]
    mirror = left_many(tab["left"], real, imag)
    return direct, mirror


def y_inverse(tab, real, imag, edge, place):
    imag, real = left_many(tab["left"], imag, real)
    start = lane_ids() < 8
    cos, sin = 2.0 * tab.turn("turn_y", 0), 2.0 * tab.turn("turn_y", 1)
    parts = [
        [p * cos - q * sin for p, q in zip(real, imag)],
        [p * sin + q * cos for p, q in zip(real, imag)],
    ]
    for part, values in zip(parts, edge):
        for xh in range(4):
            part[xh] = jnp.where(start, roll(values, -(32 * xh + 8 * place)), part[xh])
    return right_many(tab["inverse_y"], *parts)


def edge_rows(tab, sets):
    lane = lane_ids()
    packed = [0.0, 0.0]
    for place, both in enumerate(sets):
        for part, blocks in enumerate(both):
            for xh in range(4):
                mine = (lane >> 3) == 4 * xh + place
                moved = roll(blocks[xh], 32 * xh + 8 * place)
                packed[part] = jnp.where(mine, moved, packed[part])
    first, second = left_many(tab["left_edge"], [packed[0]], [packed[1]])
    return first[0], second[0]


def load(ref, index, count):
    return ref[pl.ds(index, 128, stride=count), :]


def store(ref, index, count, block):
    ref[pl.ds(index, 128, stride=count), :] = block


def load_set(ref, base, count):
    real = [load(ref, base + k, count) for k in range(4)]
    imag = [load(ref, base + 4 + k, count) for k in range(4)]
    return real, imag


def store_set(ref, base, count, real, imag):
    for k in range(4):
        store(ref, base + k, count, real[k])
        store(ref, base + 4 + k, count, imag[k])


def block(ref, index):
    return ref[128 * index : 128 * index + 128, :]


def put(ref, index, value):
    ref[128 * index : 128 * index + 128, :] = value


def rank_here():
    return lax.axis_index("gx") * lax.axis_size("gy") + lax.axis_index("gy")


class Rows:
    def __init__(self, rank, group, quarter):
        lane = lax.broadcasted_iota(jnp.int32, (1, 128), 1)
        slot = 4 * quarter + ((lane >> 3) & 3)
        if group == 1:
            slot = jnp.where(slot == 0, 16, 32 - slot)
        if group == 2:
            slot = jnp.where((slot == 0) & (rank >= 64), 16, slot)
        row = 32 * rank + slot
        my = jnp.where(row < GRID // 2, row, row - GRID)
        self.my = my
        self.square = (my * my).astype(jnp.float32)
        self.slope = jnp.where(row == GRID // 2, 0, my).astype(jnp.float32) * unit

    def keep(self, cutoff):
        return jnp.where(jnp.abs(self.my) <= cutoff, 1.0, 0.0)

    def low(self):
        half = LOW // 2
        return jnp.where((self.my >= -half) & (self.my < half), 1.0, 0.0)


def keep_columns(tab, cutoff):
    return jnp.where(tab.turn("wave_x", 1) <= (cutoff * cutoff).astype(jnp.float32), 1.0, 0.0)


def send_fields(tab, rank, state, hidden, out_ref, count, names):
    rows = [Rows(rank, 2, q) for q in range(4)]
    across, squares = tab.turn("wave_x", 0), tab.turn("wave_x", 1)
    sources = {}
    for index in range(4):
        real, imag = state(0, index)
        if index == 0:
            upper = first_slot() & (rank >= 64)
            real, imag = [
                jnp.where(upper, other, own) for own, other in zip((real, imag), state(1, 0))
            ]
        both = squares + rows[index].square
        scale = jnp.where(both == 0.0, 0.0, (1.0 / (unit * unit)) / jnp.maximum(both, 1.0))
        sources["w", index] = real, imag
        sources["psi", index] = real * scale, imag * scale
    scale = (1.0 / (unit * unit)) / (squares + float((GRID // 2) ** 2))
    for place, name in enumerate(names):
        reals, imags = [], []
        for index in range(4):
            real, imag = sources["psi" if name in ("u", "v") else "w", index]
            factor = rows[index].slope if name in ("u", "wy") else across
            if name == "v":
                reals.append(imag * factor)
                imags.append(-real * factor)
            else:
                reals.append(-imag * factor)
                imags.append(real * factor)
        if name in ("v", "wx"):
            factor = across * scale if name == "v" else -across
            reals[0] = reals[0] + hidden[0] * factor
            imags[0] = imags[0] + hidden[1] * factor
        real, imag = x_inverse(tab, reals, imags)
        store_set(out_ref, 8 * place, count, swap4(real), swap4(imag))


def first_slot():
    return ((lane_ids() >> 3) & 3) == 0


def split_rows(tab, rank, real, imag):
    flip = tab["flip"]
    sub = row_ids()
    both = jnp.concatenate([real, imag], axis=0)
    high, low = halves(both)
    pair = jnp.concatenate([high, low], axis=1)
    twice = lambda table, axis: jnp.concatenate([table, table], axis=axis)
    lanes = jnp.concatenate([flip[:128], flip[128:256]], axis=1)
    out = dot(pair, twice(lanes, 0))
    most, top = out[:, :128], out[:, 128:]
    wide = jnp.concatenate([most[:128], most[128:]], axis=1)
    high, low = halves(wide)
    wide = dot(twice(flip[256:], 1), jnp.concatenate([high, low], axis=0))
    real_back = jnp.where(sub == 0, top[:128], wide[:, :128])
    imag_back = jnp.where(sub == 0, top[128:], wide[:, 128:])
    mine = first_slot() & (rank == 0)
    own = [
        jnp.where(mine, 0.5 * (real + real_back), real),
        jnp.where(mine, 0.5 * (imag - imag_back), imag),
    ]
    hidden = [
        jnp.where(mine, 0.5 * (imag + imag_back), 0.0),
        jnp.where(mine, 0.5 * (real_back - real), 0.0),
    ]
    return own, hidden


FIRST = ("left", "forward_y", "turn_y", "low_rows", "turn_low")
WAVES = ("left", "right_x", "turn_x", "wave_x")
START = WAVES + ("flip",)
MIDDLE = WAVES + ("half",)
FINAL = WAVES + ("coarse_rows", "coarse_turn")
ROWS = ("left", "left_edge", "forward_y", "inverse_y", "turn_y")
PRODUCT = ROWS + ("drive_spots",)
LAST = ROWS + ("coarse_y", "coarse_x")


def grid_groups(ref):
    groups = []
    for xh in range(4):
        pair = []
        for jh in range(2):
            pieces = [
                ref[8 * xh : 8 * xh + 8, 128 * j : 128 * j + 128]
                for j in range(16 * jh, 16 * jh + 16)
            ]
            pair.append(jnp.concatenate(pieces, axis=0).T)
        groups.append(pair)
    return groups


def first_kernel(*rest):
    total = 2 + len(FIRST)
    out_ref, *held, ready = rest[total + 1 :]
    copies = {}
    for name in ("rows", "forward_y", "turn_y", "left", "force", "low_rows", "turn_low"):
        k = ("rows", "force").index(name) if name in ("rows", "force") else 2 + FIRST.index(name)
        copies[name] = pltpu.make_async_copy(rest[k], held[k], ready.at[k])
        copies[name].start()
    vorticity_ref, forcing_ref = held[:2]
    tab = Tables(FIRST, held[2:])
    for name in ("rows", "forward_y", "turn_y", "left"):
        copies[name].wait()
    direct, mirror = y_forward(tab, grid_groups(vorticity_ref))
    lane, row = lane_ids(), row_ids()
    spot = (lane < 8) & (row == 0)
    real, imag = direct
    imag = [
        jnp.where(spot, jnp.broadcast_to(p[64:65, :], (128, 128)), q)
        for p, q in zip(real, imag)
    ]
    store_set(out_ref, 0, 17, real, imag)
    store_set(out_ref, 8, 17, *mirror)
    for name in ("force", "low_rows", "turn_low"):
        copies[name].wait()
    groups = grid_groups(forcing_ref)
    values = jnp.concatenate([g[k] for g in groups for k in range(2)], axis=1)
    high, low = halves(values)
    out = dot(thrice(tab["low_rows"], 1), jnp.concatenate([high, low, high], axis=0))
    lane, row = lane_ids(), row_ids()
    sign = jnp.where((row & 1) == 0, 1.0, -1.0)
    cos, sin = tab.turn("turn_low", 0), tab.turn("turn_low", 1)
    packed = jnp.zeros((128, 128), jnp.float32)
    for xh in range(4):
        at = 256 * xh
        real = out[:128, at : at + 128] + sign * out[:128, at + 128 : at + 256]
        imag = out[128:, at : at + 128] + sign * out[128:, at + 128 : at + 256]
        for part, value in enumerate(turned(real, imag, cos, sin)):
            for shift in (64, 32, 16, 8):
                value = value + roll(value, shift)
            mine = ((lane >> 5) == xh) & (((lane >> 3) & 3) == part)
            packed = jnp.where(mine, value, packed)
    store(out_ref, 16, 17, packed)


def start_kernel(in_ref, *rest):
    tab = Tables(START, rest)
    state_ref, out_ref = rest[len(START) :]
    rank = rank_here()
    for group in range(2):
        real, imag = x_forward(tab, *load_set(in_ref, 8 * group, 17))
        if group == 0:
            (real[0], imag[0]), hidden = split_rows(tab, rank, real[0], imag[0])
            put(state_ref, 16, hidden[0])
            put(state_ref, 17, hidden[1])
        for q in range(4):
            put(state_ref, 8 * group + 2 * q, real[q])
            put(state_ref, 8 * group + 2 * q + 1, imag[q])
    row = load(in_ref, 16, 17)
    lane = lane_ids()
    part = (lane >> 3) & 3
    real = jnp.where(part == 0, row, jnp.where(part == 1, roll(row, 8), 0.0))
    imag = jnp.where(part == 0, roll(row, -8), jnp.where(part == 1, -row, 0.0))
    real, imag = x_plain(tab, [real], [imag])

    packed = jnp.zeros((128, 128), jnp.float32)
    for which, source in enumerate((real[0], imag[0])):
        for spot, origin in enumerate((0, 103, 8, 111)):
            at = 4 * which + spot
            packed = jnp.where(lane == at, roll(source, at - origin), packed)
    store(out_ref, 24, 25, packed)

    state = lambda group, q: (
        block(state_ref, 8 * group + 2 * q),
        block(state_ref, 8 * group + 2 * q + 1),
    )
    hidden = block(state_ref, 16), block(state_ref, 17)
    send_fields(tab, rank, state, hidden, out_ref, 25, ("u", "v", "wx"))


def product_one(tab, in_ref, count, edge, place):
    real, imag = load_set(in_ref, 8 * place, count)
    return y_inverse(tab, real, imag, edge, place)


def drive_rows(tab, values):
    columns = values.T
    pick = lambda index: jnp.broadcast_to(columns[index : index + 1, :], (8, 128))
    plus = swap4([pick(4 * part + k) for part in range(2) for k in range(2)])
    minus = swap4([pick(4 * part + 2 + k) for part in range(2) for k in range(2)])
    sub = lax.broadcasted_iota(jnp.int32, (8, 128), 0)
    start = (lax.broadcasted_iota(jnp.int32, (8, 128), 1) & 31) == 0
    top = jnp.zeros((8, 128), jnp.float32)
    bottom = jnp.zeros((8, 128), jnp.float32)
    for k in range(4):
        top = jnp.where(sub == k, plus[k], top)
        after = minus[k + 1] if k < 3 else 0.0
        bottom = jnp.where(sub == 7 - k, jnp.where(start, after, minus[k]), bottom)
    spots = tab["drive_spots"]
    made = []
    for values, table in ((top, spots[:128]), (bottom, spots[128:])):
        high, low = halves(values)
        made.append(dot(high, table) + dot(low, table))
    return jnp.concatenate([made[0], jnp.zeros((112, 128), jnp.float32), made[1]], axis=0)


def product_first_kernel(in_ref, local_ref, *rest):
    tab = Tables(PRODUCT, rest)
    out_ref = rest[len(PRODUCT)]
    store(out_ref, 16, 17, drive_rows(tab, load(in_ref, 24, 25)))
    lane = lane_ids()
    upper = (lane < 8) & (row_ids() >= 64)
    row = 32 * row_ids() + jnp.where(upper, 16, lane >> 3)
    slope = jnp.where(row < GRID // 2, row, row - GRID)
    slope = jnp.where(row == GRID // 2, 0, slope).astype(jnp.float32) * unit
    real, imag = load_set(local_ref, 0, 17)
    other_real, other_imag = load_set(local_ref, 8, 17)
    own = (
        [-slope * jnp.where(upper, b, a) for a, b in zip(imag, other_imag)],
        [slope * jnp.where(upper, b, a) for a, b in zip(real, other_real)],
    )
    last = edge_rows(tab, [load_set(in_ref, 8 * k, 25) for k in range(3)] + [own])
    u0, u1 = product_one(tab, in_ref, 25, last, 0)
    x0, x1 = product_one(tab, in_ref, 25, last, 2)
    sum0 = [a * b for a, b in zip(u0, x0)]
    sum1 = [a * b for a, b in zip(u1, x1)]
    y0, y1 = y_inverse(tab, *own, last, 3)
    v0, v1 = product_one(tab, in_ref, 25, last, 1)
    sum0 = [s + a * b for s, a, b in zip(sum0, v0, y0)]
    sum1 = [s + a * b for s, a, b in zip(sum1, v1, y1)]
    direct, mirror = y_forward(tab, list(zip(sum0, sum1)))
    store_set(out_ref, 0, 17, *direct)
    store_set(out_ref, 8, 17, *mirror)


def product_kernel(in_ref, *rest):
    tab = Tables(LAST, rest)
    out_ref, mixed_ref = rest[len(LAST) :]
    got = load(in_ref, 32, 33)
    mixed_ref[0:4, :] = got[0:4, :]
    mixed_ref[4:8, :] = got[124:128, :]
    last = edge_rows(tab, [load_set(in_ref, 8 * k, 33) for k in range(4)])
    sum0, sum1 = None, None
    for one, two in ((0, 2), (1, 3)):
        a0, a1 = product_one(tab, in_ref, 33, last, one)
        b0, b1 = product_one(tab, in_ref, 33, last, two)
        made0 = [a * b for a, b in zip(a0, b0)]
        made1 = [a * b for a, b in zip(a1, b1)]
        sum0 = made0 if sum0 is None else [s + m for s, m in zip(sum0, made0)]
        sum1 = made1 if sum1 is None else [s + m for s, m in zip(sum1, made1)]
    direct, mirror = y_forward(tab, list(zip(sum0, sum1)))
    store_set(out_ref, 0, 20, *direct)
    store_set(out_ref, 8, 20, *mirror)
    pieces = []
    for xh in range(4):
        for part in (direct[0], direct[1], mirror[0], mirror[1]):
            pieces.append(part[xh][0:8, :])
    across = jnp.concatenate(pieces, axis=0).T
    made = [
        swap4([across[8 * t : 8 * t + 8, :] for t in range(4 * tq, 4 * tq + 4)])
        for tq in range(4)
    ]
    values = jnp.concatenate(
        [jnp.concatenate([made[tq][xh] for tq in range(4)], axis=1) for xh in range(4)],
        axis=0,
    )
    high, low = halves(values)
    points = dot(
        jnp.concatenate([high, low, high], axis=1), thrice(tab["coarse_y"], 0)
    )
    flip = lax.broadcasted_iota(jnp.int32, (32, LOW), 1) & 1
    edge = jnp.where(flip == 0, 1.0, -1.0) * values[:, 12:13]
    high, low = halves(jnp.concatenate([points, edge], axis=0))
    share = dot(
        tab["coarse_x"], jnp.concatenate([high, low, high, jnp.zeros_like(low)], axis=0)
    )
    for odd in range(2):
        for side in range(2):
            piece = share[128 * odd : 128 * odd + 128, 128 * side : 128 * side + 128]
            piece = pltpu.roll(piece, rank_here(), 0)
            store(out_ref, 16 + 2 * odd + side, 20, piece)


def shelled(rank, values, radii):
    lane = lane_ids()
    side, spot = (lane >> 5) & 1, lane & 7
    slot = 4 * (spot & 3) + ((lane >> 3) & 3)
    slot = jnp.where(spot < 4, slot, jnp.where(slot == 0, 16, 32 - slot))
    my = 32 * rank + slot
    my = jnp.where(my < GRID // 2, my, my - GRID)
    mx = row_ids() - 128 * side
    squares = mx * mx + my * my
    mask = None
    for radius in radii:
        inside = (radius * radius <= squares) & (squares < (radius + 1) * (radius + 1))
        mask = inside if mask is None else mask | inside
    return jnp.where(mask, values, 0.0)


def fetch(ready, pairs):
    copies = [
        pltpu.make_async_copy(source, target, ready.at[k])
        for k, (source, target) in enumerate(pairs)
    ]
    for copy in copies:
        copy.start()
    return copies


def middle_kernel(cutoff_from, shells_from, in_ref, state_ref, *rest):
    tab = Tables(MIDDLE, rest)
    ahead_ref, out_ref, next_ref, cutoff_ref, shells_ref, ready = rest[len(MIDDLE) :]
    copies = fetch(ready, ((cutoff_from, cutoff_ref), (shells_from, shells_ref)))
    rank = rank_here()
    lane = lane_ids()
    spectra = [x_forward(tab, *load_set(in_ref, 8 * group, 17)) for group in range(2)]
    for copy in copies:
        copy.wait()
    cutoff = cutoff_ref[0]
    forcing = shelled(rank, load(in_ref, 16, 17), [shells_ref[k] for k in range(SHELLS)])
    first_spots = (lane < 32) & ((lane & 7) == 0)
    last_spots = (lane >= 96) & ((lane & 7) == 7)
    keep_x = keep_columns(tab, cutoff)
    squares, low_x = tab.turn("wave_x", 1), tab.turn("wave_x", 2)
    low0 = [0.0, 0.0]
    low1 = [0.0, 0.0]
    for group in range(2):
        real, imag = spectra[group]
        for q in range(4):
            rows = Rows(rank, group, q)
            keep = keep_x * rows.keep(cutoff)
            low = low_x * rows.low()
            damp = (viscosity * unit * unit) * (squares + rows.square)
            spot = 4 * group + q
            mine = (lane < 32) & ((lane & 7) == spot)
            for part, term in enumerate((real[q], imag[q])):
                place = 8 * group + 2 * q + part
                now = block(state_ref, place)
                drive = jnp.where(first_spots, roll(forcing, -64 * part - spot), 0.0)
                drive = jnp.where(
                    last_spots, roll(forcing, 71 - 64 * part - spot), drive
                )
                slope = drive - keep * term - damp * now
                after = now + time_step * slope
                if place < 10:
                    put(next_ref, place, after)
                rest_slope = slope + drive - damp * after
                change = 0.5 * time_step * rest_slope
                lifted = now + change + (coarse_ratio * low) * change
                put(ahead_ref, place, lifted)
                lifted = low * lifted
                low0[part] = jnp.where(mine, roll(lifted, spot), low0[part])
                low1[part] = jnp.where(mine, roll(lifted, 25 + spot), low1[part])
    even = [a + b for a, b in zip(low0, low1)]
    odd = [a - b for a, b in zip(low0, low1)]
    cos, sin = tab.turn("half", 0), tab.turn("half", 1)
    odd = [odd[0] * cos - odd[1] * sin, odd[0] * sin + odd[1] * cos]
    both = [jnp.where(lane < 32, e, roll(o, 32)) for e, o in zip(even, odd)]
    both = [jnp.where(lane < 64, b, 0.0) for b in both]
    second, first = left_many(tab["left"], [both[1]], [both[0]])
    store(out_ref, 32, 33, jnp.where(lane < 64, first[0], roll(second[0], 64)))
    state = lambda group, q: (
        block(next_ref, 8 * group + 2 * q),
        block(next_ref, 8 * group + 2 * q + 1),
    )
    damp = (viscosity * unit * unit) * (squares + float((GRID // 2) ** 2))
    fade = 1.0 - time_step * damp
    hidden = block(state_ref, 16) * fade, block(state_ref, 17) * fade
    send_fields(tab, rank, state, hidden, out_ref, 33, ("u", "v", "wx", "wy"))


def final_kernel(cutoff_from, in_ref, ahead_ref, mixed_ref, *rest):
    tab = Tables(FINAL, rest)
    out_ref, points_ref, held_ref, cutoff_ref, ready, done_ref = rest[len(FINAL) :]
    (copy,) = fetch(ready, ((cutoff_from, cutoff_ref),))
    rank = rank_here()
    spectra = [x_forward(tab, *load_set(in_ref, 8 * group, 20)) for group in range(2)]
    copy.wait()
    cutoff = cutoff_ref[0]
    keep_x = keep_columns(tab, cutoff) * (0.5 * time_step)
    low_x = tab.turn("wave_x", 2) * coarse_ratio
    copies = []
    for group in range(2):
        factors = []
        for q in range(4):
            rows = Rows(rank, group, q)
            factor = keep_x * rows.keep(cutoff)
            factors.append(factor + factor * (low_x * rows.low()))
        for part in range(2):
            for q in range(4):
                lifted = block(ahead_ref, 8 * group + 2 * q + part)
                flipped = (lifted - factors[q] * spectra[group][part][q]).T
                for kh in range(4):
                    for slot in range(4):
                        at = 32 * kh + 8 * slot
                        number = 4 * q + slot
                        if group == 1:
                            number = 16 if number == 0 else 32 - number
                        start = 1024 * part + 256 * (number // 8) + 64 * kh + number % 8
                        held_ref[pl.ds(start, 8, stride=8), :] = flipped[at : at + 8, :]
            spot = slice(1024 * part + 512 * group, 1024 * part + 512 * group + 512)
            copies.append(
                pltpu.make_async_copy(
                    held_ref.at[spot], out_ref.at[spot], done_ref.at[2 * group + part]
                )
            )
            copies[-1].start()
    mixed = mixed_ref[...]
    high, low = halves(jnp.concatenate([mixed, roll(mixed, -32)], axis=0))
    out = dot(
        jnp.concatenate([high, low, high], axis=1), thrice(tab["coarse_rows"], 0)
    )
    turn = tab["coarse_turn"]
    for odd in range(2):
        rows = out[8 * odd : 8 * odd + 8]
        rows = rows[:, :LOW] * turn[:8] + rows[:, LOW:] * turn[8:]
        line = jnp.sum(rows, axis=0, keepdims=True)
        for side in range(2):
            total = jnp.sum(load(in_ref, 16 + 2 * odd + side, 20), axis=0, keepdims=True)
            at = slice(128 * side, 128 * side + 128)
            points_ref[odd : odd + 1, at] = line[:, at] + total
    for copy in copies:
        copy.wait()


VMEM = pl.BlockSpec(memory_space=pltpu.VMEM)


HBM = pl.BlockSpec(memory_space=pltpu.HBM)


def call(kernel, name, outs, args, far=(), out_specs=None, scratch=()):
    far = tuple(
        a if a.ndim == 1 else pltpu.with_memory_space_constraint(a, pltpu.HBM) for a in far
    )
    return pl.pallas_call(
        kernel,
        name=name,
        out_shape=[jax.ShapeDtypeStruct(shape, jnp.float32) for shape in outs],
        in_specs=[HBM] * len(far) + [VMEM] * len(args),
        out_specs=out_specs or [VMEM] * len(outs),
        scratch_shapes=list(scratch),
        compiler_params=pltpu.CompilerParams(vmem_limit_bytes=VMEM_LIMIT * 1024 * 1024),
    )(*far, *args)


def near(array):
    return pltpu.with_memory_space_constraint(array, pltpu.VMEM)


def exchange(buffer, count):
    cut = buffer.reshape(128, 1, count * 128)
    cut = lax.all_to_all(cut, AXES, split_axis=0, concat_axis=0, tiled=True)
    return cut.reshape(128 * count, 128)


def body(vorticity_grid, forcing_grid, cutoff, forcing_shells):
    made = {name: jnp.asarray(table) for name, table in tables().items()}
    tabs = lambda names: tuple(made[name] for name in names)
    spectrum = (16 * 128, 128)
    args = (vorticity_grid, forcing_grid) + tabs(FIRST)
    (sent,) = call(
        first_kernel,
        "first",
        [(128 * 17, 128)],
        (),
        args + (cutoff,),
        scratch=[pltpu.VMEM(a.shape, a.dtype) for a in args]
        + [pltpu.SemaphoreType.DMA((len(args),))],
    )
    got = exchange(sent, 17)
    state, fields = call(
        start_kernel, "start", [(18 * 128, 128), (128 * 25, 128)], (got,) + tabs(START)
    )
    got = exchange(fields, 25)
    (term,) = call(
        product_first_kernel, "product_first", [(128 * 17, 128)], (got, near(sent)) + tabs(PRODUCT)
    )
    got = exchange(term, 17)
    ahead, fields = call(
        middle_kernel,
        "middle",
        [spectrum, (128 * 33, 128)],
        (got, near(state)) + tabs(MIDDLE),
        (cutoff, forcing_shells),
        scratch=[
            pltpu.VMEM((10 * 128, 128), jnp.float32),
            pltpu.SMEM((1,), jnp.int32),
            pltpu.SMEM((SHELLS,), jnp.int32),
            pltpu.SemaphoreType.DMA((2,)),
        ],
    )
    got = exchange(fields, 33)
    term, mixed = call(
        product_kernel, "product", [(128 * 20, 128), (8, 128)], (got,) + tabs(LAST)
    )
    got = exchange(term, 20)
    lifted, coarse = call(
        final_kernel,
        "final",
        [(2048, 128), (2, LOW)],
        (got, near(ahead), mixed) + tabs(FINAL),
        (cutoff,),
        out_specs=[HBM, VMEM],
        scratch=[
            pltpu.VMEM((2048, 128), jnp.float32),
            pltpu.SMEM((1,), jnp.int32),
            pltpu.SemaphoreType.DMA((1,)),
            pltpu.SemaphoreType.DMA((4,)),
        ],
    )
    lifted = lifted.reshape(2, 4, 32, 8, 128).transpose(0, 1, 3, 2, 4).reshape(2, 32, GRID)
    return lifted, coarse


def solution(mesh):
    placed = (P(AXES, None), P(AXES, None), P(), P())
    return jax.shard_map(
        body,
        mesh=mesh,
        in_specs=placed,
        out_specs=(P(None, AXES, None), P(AXES, None)),
        check_vma=False,
    )
```
